32 devices in a mesh: slab: 8 (over z, x), sub: 4 (over y, core).
Axes of the slice: x: 2, y: 2, z: 4, core: 2. Of those that a mesh axis runs over, the one named last changes fastest.
Arguments:
- values: float32 [768, 2, 128, 256], P(('slab', 'sub')), may hold values from -0.25 to 0.25
- block_ids: int32 [768, 2], P(('slab', 'sub')), may hold values from 0 to 383, as said below
- tile_counts: int32 [8, 4], P('slab', 'sub'), may hold values from 8 to 24, as said below
- right_side: float32 [768, 128], P(('slab', 'sub')), may hold values from -18 to 18
Outputs:
- solution: float32 [384, 256], P(('slab', 'sub'))
- residual: float32 [768, 128], P(('slab', 'sub'))
The draws below stay inside these ranges and needn't reach their ends.
Inputs may be any that keep to these rules, and one draw needn't show every extreme that they name: `block_ids`: every block id names a node block held by a device of the row tile's own slab or of a slab one index of slab away; the first coupled block of each tile lies in its own slab. Block b is held by device b div 12. `tile_counts`: some device has all 24 slots live in every draw.
All inputs are finite; a program needn't handle non-finite values.
Results may differ from the reference program's by a relative error of at most 0.0003.
Values sent between devices are 32-bit elements; how exact they have to be, the bound alone decides.
A program may use at most 64 MiB of HBM per device.

```python
import jax
import jax.numpy as jnp
from jax import lax

BLOCK = 256
TILE_ROWS = 128
COUPLED = 2
ITERS = 4
TILES_DEV = 24
NB_DEV = 12
TILES = 768
NBLOCKS = 384
N_SLAB = 8
N_SUB = 4


def draw_block_ids(key, part):
    tile_slab = jnp.arange(TILES, dtype=jnp.int32) // TILES_DEV // N_SUB
    offset = jax.random.randint(jax.random.fold_in(key, 11), (TILES, COUPLED), -1, 2)
    first_slot = jnp.arange(COUPLED, dtype=jnp.int32)[None, :] == 0
    offset = jnp.where(first_slot, 0, offset)
    other_slab = jnp.clip(tile_slab[:, None] + offset, 0, N_SLAB - 1)
    owner_sub = jax.random.randint(jax.random.fold_in(key, 12), (TILES, COUPLED), 0, N_SUB)
    slot_index = jax.random.randint(jax.random.fold_in(key, 13), (TILES, COUPLED), 0, NB_DEV)
    return ((other_slab * N_SUB + owner_sub) * NB_DEV + slot_index).astype(jnp.int32)


def draw_tile_counts(key, part):
    lowest = TILES_DEV // 3
    counts = jax.random.randint(jax.random.fold_in(key, 21), (N_SLAB * N_SUB,), lowest, TILES_DEV + 1)
    fuller = jax.random.randint(jax.random.fold_in(key, 22), (), 0, N_SLAB * N_SUB)
    counts = jnp.where(jnp.arange(N_SLAB * N_SUB, dtype=jnp.int32) == fuller, TILES_DEV, counts)
    return counts.reshape(N_SLAB, N_SUB).astype(jnp.int32)


def draw_right_side(key, part):
    position = jnp.arange(TILES, dtype=jnp.float32) / max(TILES - 1, 1)
    base = jnp.clip(jax.random.normal(jax.random.fold_in(key, 32), (TILES, TILE_ROWS), jnp.float32), -6.0, 6.0)
    rising = 1.0 + 2.0 * position
    return (base * rising[:, None]).astype(jnp.float32)


def steps_of(stream_key, extent, shards, smallest, top_value):
    level = 1.0
    for dim, parts in shards:
        heights = jax.random.uniform(jax.random.fold_in(jax.random.fold_in(stream_key, 6), dim), (parts,), jnp.float32, smallest / len(shards), top_value / len(shards))
        level = level * jnp.repeat(jnp.exp(heights), extent[dim] // parts).reshape((-1,) + (1,) * (len(extent) - 1 - dim))
    return level


def bell_draw(key, extent, width, reach, split=(), held_as=jnp.bfloat16):
    entries = jax.random.normal(key, extent, jnp.float32) * width
    if len(split) > 0:
        entries = steps_of(key, extent, split, -0.22, 0.18) * entries
    return jnp.clip(entries, min=-reach, max=reach).astype(held_as)


def setup_inputs(seed: int = 0) -> dict:
    key_list = jax.random.split(jax.random.key(seed), 5)
    return {
        "values": bell_draw(key_list[0], (TILES, COUPLED, TILE_ROWS, BLOCK), (COUPLED * BLOCK) ** -0.5, 0.25, ((0, 32),), jnp.float32),
        "block_ids": draw_block_ids(jax.random.fold_in(key_list[4], 71), 0),
        "tile_counts": draw_tile_counts(jax.random.fold_in(key_list[4], 71), 0),
        "right_side": draw_right_side(jax.random.fold_in(key_list[4], 71), 0),
    }


precise = lax.Precision.HIGHEST


def live_mask(tile_counts):
    position = jnp.arange(TILES, dtype=jnp.int32)
    owner_dev = (position // TILES_DEV).astype(jnp.int32)
    limit = tile_counts.reshape(-1)[owner_dev]
    return ((position % TILES_DEV) < limit).astype(jnp.float32)


def forward(values, block_ids, live_tiles, field):
    picked = field[block_ids]
    image = jnp.einsum("tkij,tkj->ti", values, picked, precision=precise)
    return image * live_tiles[:, None]


def backward(values, block_ids, rows):
    terms = jnp.einsum("tkij,ti->tkj", values, rows, precision=precise)
    return jax.ops.segment_sum(terms.reshape(-1, BLOCK), block_ids.reshape(-1), num_segments=NBLOCKS)


def reference(values, block_ids, tile_counts, right_side):
    live_tiles = live_mask(tile_counts)
    squares = jnp.einsum("tkij,tkij->tkj", values, values, precision=precise) * live_tiles[:, None, None]
    col_squares = jax.ops.segment_sum(squares.reshape(-1, BLOCK), block_ids.reshape(-1), num_segments=NBLOCKS)
    jacobi = 1.0 / (1.0 + col_squares)
    solution = jnp.zeros((NBLOCKS, BLOCK), jnp.float32)
    residual = right_side * live_tiles[:, None]
    normal_res = backward(values, block_ids, residual)
    scaled = jacobi * normal_res
    direction = scaled
    rho_now = jnp.sum(normal_res * scaled)
    for iteration in range(ITERS):
        image = forward(values, block_ids, live_tiles, direction)
        step_size = rho_now / jnp.sum(image * image)
        solution = solution + step_size * direction
        residual = residual - step_size * image
        normal_res = backward(values, block_ids, residual)
        scaled = jacobi * normal_res
        rho_next = jnp.sum(normal_res * scaled)
        direction = scaled + (rho_next / rho_now) * direction
        rho_now = rho_next
    return (solution, residual)
```

```python
import functools

import jax
import jax.numpy as jnp
from jax import lax
from jax.experimental import pallas as pl
from jax.experimental.pallas import tpu as pltpu
from jax.sharding import PartitionSpec as P

ITERS = 4
NB_DEV = 12
LANES = 128
SUMS = 3
MESH = pl.DeviceIdType.MESH


def round_up(size, unit):
    return -(-size // unit) * unit


def divisor(size, *wanted):
    return next(g for g in (*wanted, 1) if size % g == 0)


def kernel(
    n_slab,
    n_sub,
    values_hbm,
    ids_hbm,
    counts_hbm,
    right_hbm,
    solution_ref,
    residual_ref,
    values,
    wid,
    selector,
    terms,
    squares,
    cols,
    rows_ref,
    first_out,
    first_in,
    part_out,
    part_in,
    field_out,
    field_in,
    scal,
    ids_smem,
    counts_smem,
    right_ref,
    small_sem,
    load_sem,
    first_send,
    first_recv,
    part_send,
    part_recv,
    field_send,
    field_recv,
    scal_send,
    scal_recv,
):
    tiles, coupled, rows, block = values.shape
    halves = block // LANES
    held = NB_DEV * halves
    n = n_slab * n_sub
    window = 3 * n_sub * held
    n_terms = terms.shape[0]
    f32 = jnp.float32
    slab = lax.axis_index("slab")
    sub = lax.axis_index("sub")
    me = slab * n_sub + sub

    kept = slab + 1 - 2 * lax.rem(slab, 2)
    own_rel = kept - slab + 1
    beyond = 2 * slab - kept
    far_rel = slab - kept + 1
    far_out = 3 * slab - 2 * kept
    far_in = 2 * kept - slab
    sends_far = jnp.logical_and(beyond >= 0, beyond < n_slab)
    takes_far = jnp.logical_and(far_in >= 0, far_in < n_slab)

    small = [
        pltpu.make_async_copy(src, dst, small_sem.at[i])
        for i, (src, dst) in enumerate(
            ((ids_hbm, ids_smem), (counts_hbm, counts_smem), (right_hbm, right_ref))
        )
    ]
    for copy in small:
        copy.start()
    loads = load_sem.shape[0]
    group = tiles // loads

    def load(g):
        part = pl.ds(g * group, group)
        return pltpu.make_async_copy(values_hbm.at[part], values.at[part], load_sem.at[g])

    for g in range(loads):
        load(g).start()

    def other(j):
        target = lax.rem(me + j, n)
        return (lax.div(target, n_sub), lax.rem(target, n_sub))

    barrier = pltpu.get_barrier_semaphore()

    @pl.loop(1, n)
    def _(j):
        pl.semaphore_signal(barrier, inc=1, device_id=other(j), device_id_type=MESH)

    n_used = tiles * coupled * halves
    if n_terms > n_used:
        terms[n_used:] = jnp.zeros((n_terms - n_used, LANES), f32)
        squares[n_used:] = jnp.zeros((n_terms - n_used, LANES), f32)

    @pl.when(jnp.logical_not(takes_far))
    def _():
        for ref in (first_in, *part_in):
            ref[2 * n_sub :] = jnp.zeros((n_sub,) + ref.shape[1:], f32)

    @pl.when(jnp.logical_not(sends_far))
    def _():
        blank = pl.ds(pl.multiple_of(far_rel * n_sub * held, 8), n_sub * held)
        for ref in field_in:
            ref[blank, :] = jnp.zeros((n_sub * held, LANES), f32)

    for copy in small:
        copy.wait()

    base = (slab - 1) * n_sub * NB_DEV
    lane = lax.broadcasted_iota(jnp.int32, (1, n_terms), 1)
    lane_tile = lane % tiles
    lane_k = lane // (halves * tiles)
    lane_h = (lane // tiles) % halves
    place = jnp.full((1, n_terms), -1, jnp.int32)
    for t in range(tiles):
        for k in range(coupled):
            at = jnp.clip((ids_smem[t, k] - base) * halves, 0, window - halves)
            wid[t, k] = at
            place = jnp.where(jnp.logical_and(lane_tile == t, lane_k == k), at + lane_h, place)
    selector[...] = (
        lax.broadcasted_iota(jnp.int32, (window, n_terms), 0) == place
    ).astype(f32).astype(jnp.bfloat16)

    def live(t):
        return jnp.where(t < counts_smem[0, 0], 1.0, 0.0).astype(f32)

    eye = (
        lax.broadcasted_iota(jnp.int32, (rows, LANES), 0)
        == lax.broadcasted_iota(jnp.int32, (rows, LANES), 1)
    ).astype(f32)

    def half(h):
        return slice(h * LANES, (h + 1) * LANES)

    def term_row(k, h, t):
        return pl.ds((k * halves + h) * tiles + t, 1)

    @pl.loop(0, tiles // group)
    def _(g):
        for i in range(group):
            t = g * group + i
            alive = right_ref[pl.ds(t, 1), :] * live(t)
            residual_ref[pl.ds(t, 1), :] = alive
            cols[t] = jnp.broadcast_to(
                jnp.sum(eye * alive, axis=1, keepdims=True), (rows, LANES)
            )

    def scatter(ref):
        full = ref[...]
        high = full.astype(jnp.bfloat16)
        low = (full - high.astype(f32)).astype(jnp.bfloat16)
        spread = jnp.dot(
            selector[...], jnp.concatenate([high, low], axis=1), preferred_element_type=f32
        )
        return (spread[:, :LANES] + spread[:, LANES:]).reshape(3 * n_sub, held, LANES)

    def mates(act):
        for step in range(1, n_sub):
            act(step)

    def remote(src, dst, send, recv, device):
        return pltpu.make_async_remote_copy(
            src_ref=src, dst_ref=dst, send_sem=send, recv_sem=recv, device_id=device, device_id_type=MESH
        )

    def part_start(out_ref, in_ref, send, recv):
        def one(pos, rel, to_slab, step):
            target = lax.rem(sub + step, n_sub)
            remote(
                out_ref.at[rel * n_sub + target],
                in_ref.at[pos * n_sub + step],
                send.at[pos // 2],
                recv.at[pos // 2],
                (to_slab, target),
            ).start()

        @pl.when(sends_far)
        def _():
            for step in range(n_sub):
                one(2, far_rel, far_out, step)

        for step in range(n_sub):
            one(0, 1, kept, step)
        mates(lambda step: one(1, own_rel, slab, step))
        in_ref[n_sub] = out_ref[own_rel * n_sub + sub]

    def field_start(src, in_ref, send, recv):
        def one(sem, rel, to_slab, step):
            target = lax.rem(sub + step, n_sub)
            at = pl.multiple_of((rel * n_sub + sub) * held, 8)
            remote(
                src, in_ref.at[pl.ds(at, held)], send.at[sem], recv.at[sem], (to_slab, target)
            ).start()

        @pl.when(takes_far)
        def _():
            for step in range(n_sub):
                one(1, kept - far_in + 1, far_in, step)

        for step in range(n_sub):
            one(0, 1, kept, step)
        mates(lambda step: one(0, own_rel, slab, step))

    def group_wait(ref, per, sem, near, far_too, recv):
        def wait(i, count):
            size = ref.at[pl.ds(0, count * per)]
            copy = remote(size, size, sem.at[i], sem.at[i], (kept, sub))
            copy.wait_recv() if recv else copy.wait_send()

        wait(0, near)
        pl.when(far_too)(lambda: wait(1, n_sub))

    near = 2 * n_sub - 1

    def scal_copy(it, j):
        row = scal.at[it, pl.ds(me, 1)]
        return remote(row, row, scal_send.at[it], scal_recv.at[it], other(j))

    def scal_start(it, row):
        scal[it, pl.ds(me, 1)] = row

        @pl.loop(1, n)
        def _(j):
            scal_copy(it, j).start()

    def scal_all(it):
        rest = scal.at[it, pl.ds(0, n - 1)]
        return remote(rest, rest, scal_send.at[it], scal_recv.at[it], other(1))

    def total(x):
        return jnp.sum(jnp.sum(x, axis=0, keepdims=True), axis=1, keepdims=True)

    lane_row = lax.broadcasted_iota(jnp.int32, (1, LANES), 1)

    def pack(parts):
        row = jnp.zeros((1, LANES), f32)
        for i, x in enumerate(parts):
            row = jnp.where(lane_row == i, total(x), row)
        return row

    def unpack(it, count):
        row = jnp.sum(scal[it], axis=0, keepdims=True)
        return [
            jnp.sum(jnp.where(lane_row == i, row, 0.0), axis=1, keepdims=True)
            for i in range(count)
        ]

    @pl.loop(0, loads)
    def _(g):
        load(g).wait()
        for i in range(group):
            t = g * group + i
            alive = live(t)
            right = cols[t]
            for k in range(coupled):
                for h in range(halves):
                    a = values[t, k, :, half(h)]
                    terms[term_row(k, h, t), :] = jnp.sum(a * right, axis=0, keepdims=True)
                    squares[term_row(k, h, t), :] = (
                        jnp.sum(a * a, axis=0, keepdims=True) * alive
                    )

    for i, ref in enumerate((terms, squares)):
        first_out[:, i] = scatter(ref)
    pl.semaphore_wait(barrier, n - 1)
    part_start(first_out, first_in, first_send, first_recv)
    group_wait(first_in, 1, first_recv, near, takes_far, True)
    sums = jnp.sum(first_in[...], axis=0)
    normal_res = sums[0]
    jacobi = 1.0 / (1.0 + sums[1])

    def own_rows(ref):
        return ref[pl.ds(pl.multiple_of((n_sub + sub) * held, 8), held), :]

    def send_field(it, field):
        field_out[it] = field
        at = pl.multiple_of((own_rel * n_sub + sub) * held, 8)
        field_start(field_out.at[it], field_in[it], field_send.at[it], field_recv.at[it])
        field_in[it][pl.ds(at, held), :] = field

    scaled = jacobi * normal_res
    kept_dir = scaled
    field = scaled
    send_field(0, field)
    scal_start(0, pack((normal_res * scaled,)))
    answer = jnp.zeros((held, LANES), f32)
    for it in range(ITERS):
        last = it == ITERS - 1
        fields = field_in[it]
        group_wait(fields, held, field_recv.at[it], near, sends_far, True)

        def forward(t):
            alive = live(t)
            m = None
            for k in range(coupled):
                for h in range(halves):
                    picked = fields[pl.ds(wid[t, k] + h, 1), :] * alive
                    product = values[t, k, :, half(h)] * picked
                    m = product if m is None else m + product
            cols[t] = jnp.broadcast_to(jnp.sum(m, axis=1, keepdims=True), (rows, LANES))

        def backward(t):
            image = cols[t]
            for k in range(coupled):
                for h in range(halves):
                    terms[term_row(k, h, t), :] = jnp.sum(
                        values[t, k, :, half(h)] * image, axis=0, keepdims=True
                    )

        step = divisor(tiles, 4, 3, 2)
        for i in range(step):
            forward(i)

        @pl.loop(1, tiles // step)
        def _(g):
            if not last:
                for i in range(step):
                    backward((g - 1) * step + i)
            for i in range(step):
                forward(g * step + i)

        if not last:
            for i in range(step):
                backward(tiles - step + i)
            part_out[it] = scatter(terms)
            part_start(part_out.at[it], part_in[it], part_send.at[it], part_recv.at[it])

        @pl.loop(0, tiles, unroll=4)
        def _(t):
            rows_ref[pl.ds(t, 1), :] = jnp.sum(cols[t] * eye, axis=0, keepdims=True)

        field_own = own_rows(fields)
        scal_all(it).wait_recv()
        if it == 0:
            (rho,) = unpack(0, 1)
            scaled_own = field_own
            direction = field_own
            scaled_image = rows_ref[...]
            image = scaled_image
        else:
            curve, cross, square = unpack(it, SUMS)
            step_size = rho / curve
            rho_next = rho - 2.0 * step_size * cross + step_size * step_size * square
            beta = rho_next / rho
            rho = rho_next
            answer = answer + step_size * direction
            residual_ref[...] = residual_ref[...] - step_size * image
            scaled = scaled - step_size * field
            kept_dir = scaled + beta * kept_dir
            scaled_own = scaled_own - step_size * field_own
            direction = scaled_own + beta * direction
            scaled_image = scaled_image - step_size * rows_ref[...]
            image = scaled_image + beta * image

        if last:
            scal_start(ITERS, pack((image * image,)))
        else:
            group_wait(part_in[it], 1, part_recv.at[it], near, takes_far, True)
            spread = jnp.sum(part_in[it][...], axis=0)
            if it == 0:
                scaled_back = spread
                back = spread
            else:
                scaled_back = scaled_back - step_size * spread
                back = scaled_back + beta * back
            field = jacobi * back
            send_field(it + 1, field)
            scal_start(it + 1, pack((kept_dir * back, scaled * back, back * field)))

    scal_all(ITERS).wait_recv()
    (curve,) = unpack(ITERS, 1)
    step_size = rho / curve
    answer = answer + step_size * direction
    residual_ref[...] = residual_ref[...] - step_size * image
    rows_ref[:held] = answer
    for h in range(halves):
        solution_ref[:, half(h)] = rows_ref[pl.ds(h, NB_DEV, stride=halves), :]

    group_wait(first_in, 1, first_send, near, sends_far, False)
    for it in range(ITERS):
        group_wait(field_in[it], held, field_send.at[it], near, takes_far, False)
        if it < ITERS - 1:
            group_wait(part_in[it], 1, part_send.at[it], near, sends_far, False)
    for it in range(ITERS + 1):
        scal_all(it).wait_send()


def per_device(n_slab, n_sub, values, block_ids, tile_counts, right_side):
    tiles, coupled, rows, block = values.shape
    halves = block // LANES
    held = NB_DEV * halves
    n = n_slab * n_sub
    slots = 3 * n_sub
    window = slots * held
    n_terms = round_up(tiles * coupled * halves, LANES)
    loads = tiles // divisor(tiles, 4, 3, 2)
    f32 = jnp.float32
    vmem = pltpu.VMEM
    dma = pltpu.SemaphoreType.DMA
    whole = pl.BlockSpec(memory_space=pltpu.VMEM)
    return pl.pallas_call(
        functools.partial(kernel, n_slab, n_sub),
        out_shape=(
            jax.ShapeDtypeStruct((NB_DEV, block), f32),
            jax.ShapeDtypeStruct((tiles, rows), f32),
        ),
        in_specs=[pl.BlockSpec(memory_space=pl.ANY)] * 4,
        out_specs=(whole, whole),
        scratch_shapes=[
            vmem(values.shape, f32),
            pltpu.SMEM((tiles, coupled), jnp.int32),
            vmem((window, n_terms), jnp.bfloat16),
            vmem((n_terms, LANES), f32),
            vmem((n_terms, LANES), f32),
            vmem((tiles, rows, LANES), f32),
            vmem((tiles, LANES), f32),
            vmem((slots, 2, held, LANES), f32),
            vmem((slots, 2, held, LANES), f32),
            vmem((ITERS - 1, slots, held, LANES), f32),
            [vmem((slots, held, LANES), f32)] * (ITERS - 1),
            vmem((ITERS, held, LANES), f32),
            [vmem((window, LANES), f32)] * ITERS,
            vmem((ITERS + 1, n, LANES), f32),
            pltpu.SMEM((tiles, coupled), jnp.int32),
            pltpu.SMEM((1, 1), jnp.int32),
            vmem((tiles, rows), f32),
            dma((3,)),
            dma((loads,)),
            dma((2,)),
            dma((2,)),
            dma((ITERS - 1, 2)),
            dma((ITERS - 1, 2)),
            dma((ITERS, 2)),
            dma((ITERS, 2)),
            dma((ITERS + 1,)),
            dma((ITERS + 1,)),
        ],
        compiler_params=pltpu.CompilerParams(
            collective_id=0, has_side_effects=True, vmem_limit_bytes=48 * 1024 * 1024
        ),
    )(values, block_ids, tile_counts, right_side)


def solution(mesh):
    in_specs = (
        P(("slab", "sub"), None, None, None),
        P(("slab", "sub"), None),
        P("slab", "sub"),
        P(("slab", "sub"), None),
    )
    out_specs = (P(("slab", "sub"), None), P(("slab", "sub"), None))
    return jax.shard_map(
        functools.partial(per_device, mesh.shape["slab"], mesh.shape["sub"]),
        mesh=mesh,
        in_specs=in_specs,
        out_specs=out_specs,
        check_vma=False,
    )
```

```python
import functools

import jax
import jax.numpy as jnp
from jax import lax
from jax.experimental import pallas as pl
from jax.experimental.pallas import tpu as pltpu
from jax.sharding import PartitionSpec as P

ITERS = 4
NB_DEV = 12
LANES = 128
SUMS = 3
STEP = 4
MESH = pl.DeviceIdType.MESH


def round_up(size, unit):
    return -(-size // unit) * unit


def divisor(size, *wanted):
    return next(g for g in (*wanted, 1) if size % g == 0)


def kernel(
    n_slab,
    n_sub,
    values_hbm,
    ids_hbm,
    counts_hbm,
    right_hbm,
    solution_ref,
    residual_ref,
    values,
    wid,
    selector,
    terms,
    squares,
    cols,
    rows_ref,
    first_out,
    first_in,
    part_out,
    part_in,
    field_out,
    field_in,
    scal,
    ids_smem,
    counts_smem,
    right_ref,
    small_sem,
    load_sem,
    first_send,
    first_recv,
    part_send,
    part_recv,
    field_send,
    field_recv,
    scal_send,
    scal_recv,
    hello,
):
    tiles, coupled, rows, block = values.shape
    halves = block // LANES
    held = NB_DEV * halves
    n = n_slab * n_sub
    window = 3 * n_sub * held
    n_terms = terms.shape[0]
    f32 = jnp.float32
    slab = lax.axis_index("slab")
    sub = lax.axis_index("sub")
    me = slab * n_sub + sub

    kept = slab + 1 - 2 * lax.rem(slab, 2)
    own_rel = kept - slab + 1
    beyond = 2 * slab - kept
    far_rel = slab - kept + 1
    far_out = 3 * slab - 2 * kept
    far_in = 2 * kept - slab
    sends_far = jnp.logical_and(beyond >= 0, beyond < n_slab)
    takes_far = jnp.logical_and(far_in >= 0, far_in < n_slab)

    small = [
        pltpu.make_async_copy(src, dst, small_sem.at[i])
        for i, (src, dst) in enumerate(
            ((ids_hbm, ids_smem), (counts_hbm, counts_smem), (right_hbm, right_ref))
        )
    ]
    for copy in small:
        copy.start()
    loads = load_sem.shape[0]
    group = tiles // loads

    def load(g):
        part = pl.ds(g * group, group)
        return pltpu.make_async_copy(values_hbm.at[part], values.at[part], load_sem.at[g])

    for g in range(loads):
        load(g).start()

    def other(j):
        target = lax.rem(me + j, n)
        return (lax.div(target, n_sub), lax.rem(target, n_sub))

    barrier = pltpu.get_barrier_semaphore()

    def greet(slot, to_slab, target):
        pl.semaphore_signal(slot, inc=1, device_id=(to_slab, target), device_id_type=MESH)

    for exists, to_slab in ((sends_far, far_out), (takes_far, far_in)):

        @pl.when(exists)
        def _():
            for step in range(n_sub):
                greet(barrier, to_slab, lax.rem(sub + step, n_sub))

    for step in range(n_sub):
        greet(barrier, kept, lax.rem(sub + step, n_sub))
    for step in range(1, n_sub):
        greet(barrier, slab, lax.rem(sub + step, n_sub))

    fars = sends_far.astype(jnp.int32) + takes_far.astype(jnp.int32)
    rounds = hello.shape[0]

    def pass_on(r):
        if r > 0:
            pl.semaphore_wait(hello.at[r - 1], fars)
        if r < rounds:
            pl.when(sends_far)(lambda: greet(hello.at[r], far_out, sub))
            pl.when(takes_far)(lambda: greet(hello.at[r], far_in, sub))

    n_used = tiles * coupled * halves
    if n_terms > n_used:
        terms[n_used:] = jnp.zeros((n_terms - n_used, LANES), f32)
        squares[n_used:] = jnp.zeros((n_terms - n_used, LANES), f32)

    @pl.when(jnp.logical_not(takes_far))
    def _():
        for ref in (first_in, *part_in):
            ref[2 * n_sub :] = jnp.zeros((n_sub,) + ref.shape[1:], f32)

    @pl.when(jnp.logical_not(sends_far))
    def _():
        blank = pl.ds(pl.multiple_of(far_rel * n_sub * held, 8), n_sub * held)
        for ref in field_in:
            ref[blank, :] = jnp.zeros((n_sub * held, LANES), f32)

    for copy in small:
        copy.wait()

    base = (slab - 1) * n_sub * NB_DEV
    lane = lax.broadcasted_iota(jnp.int32, (1, n_terms), 1)
    lane_tile = lane % tiles
    lane_k = lane // (halves * tiles)
    lane_h = (lane // tiles) % halves
    place = jnp.full((1, n_terms), -1, jnp.int32)
    for t in range(tiles):
        for k in range(coupled):
            at = jnp.clip((ids_smem[k, t] - base) * halves, 0, window - halves)
            wid[t, k] = at
            place = jnp.where(jnp.logical_and(lane_tile == t, lane_k == k), at + lane_h, place)
    selector[...] = (
        lax.broadcasted_iota(jnp.int32, (window, n_terms), 0) == place
    ).astype(f32).astype(jnp.bfloat16)

    def live(t):
        return jnp.where(t < counts_smem[0, 0], 1.0, 0.0).astype(f32)

    eye = (
        lax.broadcasted_iota(jnp.int32, (rows, LANES), 0)
        == lax.broadcasted_iota(jnp.int32, (rows, LANES), 1)
    ).astype(f32)

    def half(h):
        return slice(h * LANES, (h + 1) * LANES)

    def term_row(k, h, t):
        return pl.ds((k * halves + h) * tiles + t, 1)

    @pl.loop(0, tiles // group)
    def _(g):
        for i in range(group):
            t = g * group + i
            alive = right_ref[pl.ds(t, 1), :] * live(t)
            residual_ref[pl.ds(t, 1), :] = alive
            cols[t] = jnp.broadcast_to(
                jnp.sum(eye * alive, axis=1, keepdims=True), (rows, LANES)
            )

    def scatter(ref):
        full = ref[...]
        high = full.astype(jnp.bfloat16)
        low = (full - high.astype(f32)).astype(jnp.bfloat16)
        spread = jnp.dot(
            selector[...], jnp.concatenate([high, low], axis=1), preferred_element_type=f32
        )
        return (spread[:, :LANES] + spread[:, LANES:]).reshape(3 * n_sub, held, LANES)

    def mates(act):
        for step in range(1, n_sub):
            act(step)

    def remote(src, dst, send, recv, device):
        return pltpu.make_async_remote_copy(
            src_ref=src, dst_ref=dst, send_sem=send, recv_sem=recv, device_id=device, device_id_type=MESH
        )

    def part_start(out_ref, in_ref, send, recv):
        def one(pos, rel, to_slab, step):
            target = lax.rem(sub + step, n_sub)
            remote(
                out_ref.at[rel * n_sub + target],
                in_ref.at[pos * n_sub + step],
                send.at[pos // 2],
                recv.at[pos // 2],
                (to_slab, target),
            ).start()

        @pl.when(sends_far)
        def _():
            for step in range(n_sub):
                one(2, far_rel, far_out, step)

        for step in range(n_sub):
            one(0, 1, kept, step)
        mates(lambda step: one(1, own_rel, slab, step))
        in_ref[n_sub] = out_ref[own_rel * n_sub + sub]

    def field_start(src, in_ref, send, recv):
        def one(sem, rel, to_slab, step):
            target = lax.rem(sub + step, n_sub)
            at = pl.multiple_of((rel * n_sub + sub) * held, 8)
            remote(
                src, in_ref.at[pl.ds(at, held)], send.at[sem], recv.at[sem], (to_slab, target)
            ).start()

        @pl.when(takes_far)
        def _():
            for step in range(n_sub):
                one(1, kept - far_in + 1, far_in, step)

        for step in range(n_sub):
            one(0, 1, kept, step)
        mates(lambda step: one(0, own_rel, slab, step))

    def group_wait(ref, per, sem, near, far_too, recv):
        def wait(i, count):
            size = ref.at[pl.ds(0, count * per)]
            copy = remote(size, size, sem.at[i], sem.at[i], (kept, sub))
            copy.wait_recv() if recv else copy.wait_send()

        wait(0, near)
        pl.when(far_too)(lambda: wait(1, n_sub))

    near = 2 * n_sub - 1

    def scal_copy(it, j):
        row = scal.at[it, pl.ds(me, 1)]
        return remote(row, row, scal_send.at[it], scal_recv.at[it], other(j))

    def scal_start(it, row):
        scal[it, pl.ds(me, 1)] = row

        @pl.loop(1, n, unroll=min(n - 1, 31))
        def _(j):
            scal_copy(it, j).start()

    def scal_all(it):
        rest = scal.at[it, pl.ds(0, n - 1)]
        return remote(rest, rest, scal_send.at[it], scal_recv.at[it], other(1))

    def total(x):
        return jnp.sum(jnp.sum(x, axis=0, keepdims=True), axis=1, keepdims=True)

    lane_row = lax.broadcasted_iota(jnp.int32, (1, LANES), 1)

    def pack(parts):
        row = jnp.zeros((1, LANES), f32)
        for i, x in enumerate(parts):
            row = jnp.where(lane_row == i, total(x), row)
        return row

    def unpack(it, count):
        row = jnp.sum(scal[it], axis=0, keepdims=True)
        return [
            jnp.sum(jnp.where(lane_row == i, row, 0.0), axis=1, keepdims=True)
            for i in range(count)
        ]

    def turn(x):
        rest = jnp.zeros((LANES - tiles, LANES), f32)
        return jnp.concatenate([x, rest], axis=0).T

    @pl.loop(0, loads)
    def _(g):
        load(g).wait()
        for i in range(group):
            t = g * group + i
            alive = live(t)
            right = cols[t]
            for k in range(coupled):
                for h in range(halves):
                    a = values[t, k, :, half(h)]
                    terms[term_row(k, h, t), :] = jnp.sum(a * right, axis=0, keepdims=True)
                    squares[term_row(k, h, t), :] = (
                        jnp.sum(a * a, axis=0, keepdims=True) * alive
                    )

    for i, ref in enumerate((terms, squares)):
        first_out[:, i] = scatter(ref)
    pl.semaphore_wait(barrier, 2 * n_sub - 1 + n_sub * fars)
    part_start(first_out, first_in, first_send, first_recv)
    pass_on(0)
    group_wait(first_in, 1, first_recv, near, takes_far, True)
    sums = jnp.sum(first_in[...], axis=0)
    normal_res = sums[0]
    jacobi = 1.0 / (1.0 + sums[1])

    def own_rows(ref):
        return ref[pl.ds(pl.multiple_of((n_sub + sub) * held, 8), held), :]

    def send_field(it, field):
        field_out[it] = field
        at = pl.multiple_of((own_rel * n_sub + sub) * held, 8)
        field_start(field_out.at[it], field_in[it], field_send.at[it], field_recv.at[it])
        field_in[it][pl.ds(at, held), :] = field

    scaled = jacobi * normal_res
    kept_dir = scaled
    field = scaled
    send_field(0, field)
    pass_on(1)
    rho_part = normal_res * scaled
    answer = jnp.zeros((held, LANES), f32)
    for it in range(ITERS):
        last = it == ITERS - 1
        fields = field_in[it]
        group_wait(fields, held, field_recv.at[it], near, sends_far, True)

        def reduced(t):
            alive = live(t)
            m = None
            for k in range(coupled):
                for h in range(halves):
                    picked = fields[pl.ds(wid[t, k] + h, 1), :] * alive
                    product = values[t, k, :, half(h)] * picked
                    m = product if m is None else m + product
            return jnp.broadcast_to(jnp.sum(m, axis=1, keepdims=True), (rows, LANES))

        def forward(t):
            cols[t] = reduced(t)

        def backward(t):
            image = cols[t]
            for k in range(coupled):
                for h in range(halves):
                    terms[term_row(k, h, t), :] = jnp.sum(
                        values[t, k, :, half(h)] * image, axis=0, keepdims=True
                    )

        step = divisor(tiles, STEP, 3, 2)
        if last:

            def turned_step(g, turned):
                for i in range(step):
                    t = g * step + i
                    turned = jnp.where(lane_row == t, reduced(t), turned)
                return turned

            image_t = turn(image)
            turned = turn(scaled_image)
            pushed = lax.fori_loop(0, tiles // step, turned_step, jnp.zeros((rows, LANES), f32))
        else:
            for i in range(step):
                forward(i)

            @pl.loop(1, tiles // step)
            def _(g):
                for i in range(step):
                    backward((g - 1) * step + i)
                for i in range(step):
                    forward(g * step + i)

            for i in range(step):
                backward(tiles - step + i)
            part_out[it] = scatter(terms)
            part_start(part_out.at[it], part_in[it], part_send.at[it], part_recv.at[it])

            @pl.loop(0, tiles, unroll=4)
            def _(t):
                rows_ref[pl.ds(t, 1), :] = jnp.sum(cols[t] * eye, axis=0, keepdims=True)

        field_own = own_rows(fields)
        if it == 0:
            for r in range(2, rounds + 1):
                pass_on(r)
            scaled_own = field_own
            direction = field_own
            scaled_image = rows_ref[...]
            image = scaled_image
        elif last:
            scal_all(ITERS).wait_recv()
            curve, cross = unpack(ITERS, 2)
            step_size = rho / curve
            turned = turned - step_size * pushed
            scal_start(
                it, pack((turned * turned, turned * image_t, image_t * image_t))
            )
            answer = answer + step_size * direction
            residual = residual_ref[...] - step_size * image
            scaled_own = scaled_own - step_size * field_own
            scaled_image = turned.T[:tiles]
            scal_all(it - 1).wait_recv()
            (square,) = unpack(it - 1, 1)
            rho_next = rho - 2.0 * step_size * cross + step_size * step_size * square
            beta = rho_next / rho
            rho = rho_next
            direction = scaled_own + beta * direction
            image = scaled_image + beta * image
        else:
            scal_all(it - 1).wait_recv()
            if it == 1:
                curve, cross, square, rho = unpack(it - 1, SUMS + 1)
            else:
                curve, cross, square = unpack(it - 1, SUMS)
            step_size = rho / curve
            rho_next = rho - 2.0 * step_size * cross + step_size * step_size * square
            beta = rho_next / rho
            rho = rho_next
            answer = answer + step_size * direction
            residual_ref[...] = residual_ref[...] - step_size * image
            scaled = scaled - step_size * field
            kept_dir = scaled + beta * kept_dir
            scaled_own = scaled_own - step_size * field_own
            direction = scaled_own + beta * direction
            scaled_image = scaled_image - step_size * rows_ref[...]
            image = scaled_image + beta * image

        if it == ITERS - 2:
            scal_start(ITERS, pack((image * image, scaled_image * image)))
        if not last:
            group_wait(part_in[it], 1, part_recv.at[it], near, takes_far, True)
            spread = jnp.sum(part_in[it][...], axis=0)
            if it == 0:
                scaled_back = spread
                back = spread
            else:
                scaled_back = scaled_back - step_size * spread
                back = scaled_back + beta * back
            field = jacobi * back
            send_field(it + 1, field)
            parts = (kept_dir * back, scaled * back, back * field)
            if it == 0:
                parts = parts + (rho_part,)
            scal_start(it, pack(parts[2:] if it == ITERS - 2 else parts))

    scal_all(ITERS - 1).wait_recv()
    new, mixed, old = unpack(ITERS - 1, SUMS)
    step_size = rho / (new + 2.0 * beta * mixed + beta * beta * old)
    answer = answer + step_size * direction
    residual_ref[...] = residual - step_size * image
    rows_ref[:held] = answer
    for h in range(halves):
        solution_ref[:, half(h)] = rows_ref[pl.ds(h, NB_DEV, stride=halves), :]

    group_wait(first_in, 1, first_send, near, sends_far, False)
    for it in range(ITERS):
        group_wait(field_in[it], held, field_send.at[it], near, takes_far, False)
        if it < ITERS - 1:
            group_wait(part_in[it], 1, part_send.at[it], near, sends_far, False)
    for it in range(ITERS + 1):
        scal_all(it).wait_send()


def per_device(n_slab, n_sub, values, block_ids, tile_counts, right_side):
    tiles, coupled, rows, block = values.shape
    halves = block // LANES
    held = NB_DEV * halves
    n = n_slab * n_sub
    slots = 3 * n_sub
    window = slots * held
    n_terms = round_up(tiles * coupled * halves, LANES)
    loads = tiles // divisor(tiles, 4, 3, 2)
    f32 = jnp.float32
    vmem = pltpu.VMEM
    dma = pltpu.SemaphoreType.DMA
    whole = pl.BlockSpec(memory_space=pltpu.VMEM)
    return pl.pallas_call(
        functools.partial(kernel, n_slab, n_sub),
        out_shape=(
            jax.ShapeDtypeStruct((NB_DEV, block), f32),
            jax.ShapeDtypeStruct((tiles, rows), f32),
        ),
        in_specs=[pl.BlockSpec(memory_space=pltpu.HBM)] * 4,
        out_specs=(whole, whole),
        scratch_shapes=[
            vmem(values.shape, f32),
            pltpu.SMEM((tiles, coupled), jnp.int32),
            vmem((window, n_terms), jnp.bfloat16),
            vmem((n_terms, LANES), f32),
            vmem((n_terms, LANES), f32),
            vmem((tiles, rows, LANES), f32),
            vmem((tiles, LANES), f32),
            vmem((slots, 2, held, LANES), f32),
            vmem((slots, 2, held, LANES), f32),
            vmem((ITERS - 1, slots, held, LANES), f32),
            [vmem((slots, held, LANES), f32)] * (ITERS - 1),
            vmem((ITERS, held, LANES), f32),
            [vmem((window, LANES), f32)] * ITERS,
            vmem((ITERS + 1, n, LANES), f32),
            pltpu.SMEM((coupled, tiles), jnp.int32),
            pltpu.SMEM((1, 1), jnp.int32),
            vmem((tiles, rows), f32),
            dma((3,)),
            dma((loads,)),
            dma((2,)),
            dma((2,)),
            dma((ITERS - 1, 2)),
            dma((ITERS - 1, 2)),
            dma((ITERS, 2)),
            dma((ITERS, 2)),
            dma((ITERS + 1,)),
            dma((ITERS + 1,)),
            pltpu.SemaphoreType.REGULAR((max(1, n_slab // 2 - 1),)),
        ],
        compiler_params=pltpu.CompilerParams(
            collective_id=0, has_side_effects=True, vmem_limit_bytes=48 * 1024 * 1024
        ),
    )(values, block_ids.T, tile_counts, right_side)


def solution(mesh):
    in_specs = (
        P(("slab", "sub"), None, None, None),
        P(("slab", "sub"), None),
        P("slab", "sub"),
        P(("slab", "sub"), None),
    )
    out_specs = (P(("slab", "sub"), None), P(("slab", "sub"), None))
    return jax.shard_map(
        functools.partial(per_device, mesh.shape["slab"], mesh.shape["sub"]),
        mesh=mesh,
        in_specs=in_specs,
        out_specs=out_specs,
        check_vma=False,
    )
```

```python
import functools

import jax
import jax.numpy as jnp
from jax import lax
from jax.experimental import pallas as pl
from jax.experimental.pallas import tpu as pltpu
from jax.sharding import PartitionSpec as P

ITERS = 4
NB_DEV = 12
LANES = 128
SUMS = 3
STEP = 12
MESH = pl.DeviceIdType.MESH


def round_up(size, unit):
    return -(-size // unit) * unit


def divisor(size, *wanted):
    return next(g for g in (*wanted, 1) if size % g == 0)


def kernel(
    n_slab,
    n_sub,
    values_hbm,
    ids_hbm,
    counts_hbm,
    right_hbm,
    solution_ref,
    residual_ref,
    values,
    wid,
    selector,
    terms,
    squares,
    cols,
    rows_ref,
    first_out,
    first_in,
    part_out,
    part_in,
    field_out,
    field_in,
    scal,
    ids_smem,
    counts_smem,
    right_ref,
    small_sem,
    load_sem,
    first_send,
    first_recv,
    part_send,
    part_recv,
    field_send,
    field_recv,
    scal_send,
    scal_recv,
    hello,
    jacobi,
    scaled,
    kept_dir,
    scaled_back,
    back,
    rho_row,
):
    tiles, coupled, rows, block = values.shape
    halves = block // LANES
    held = NB_DEV * halves
    n = n_slab * n_sub
    window = 3 * n_sub * held
    n_terms = terms.shape[0]
    f32 = jnp.float32
    slab = lax.axis_index("slab")
    sub = lax.axis_index("sub")
    me = slab * n_sub + sub
    pairs = n_sub // 2
    span = 2 * held
    pair = lax.div(sub, 2)
    sums_here = lax.rem(sub, 2) == 1
    rests_here = lax.rem(sub, 2) == 0

    kept = slab + 1 - 2 * lax.rem(slab, 2)
    own_rel = kept - slab + 1
    beyond = 2 * slab - kept
    far_rel = slab - kept + 1
    far_out = 3 * slab - 2 * kept
    far_in = 2 * kept - slab
    sends_far = jnp.logical_and(beyond >= 0, beyond < n_slab)
    takes_far = jnp.logical_and(far_in >= 0, far_in < n_slab)

    small = [
        pltpu.make_async_copy(src, dst, small_sem.at[i])
        for i, (src, dst) in enumerate(
            ((ids_hbm, ids_smem), (counts_hbm, counts_smem), (right_hbm, right_ref))
        )
    ]
    for copy in small:
        copy.start()
    loads = load_sem.shape[0]
    group = tiles // loads

    def load(g):
        part = pl.ds(g * group, group)
        return pltpu.make_async_copy(values_hbm.at[part], values.at[part], load_sem.at[g])

    for g in range(loads):
        load(g).start()

    def other(j):
        target = lax.rem(me + j, n)
        return (lax.div(target, n_sub), lax.rem(target, n_sub))

    barrier = pltpu.get_barrier_semaphore()

    def greet(slot, to_slab, target):
        pl.semaphore_signal(slot, inc=1, device_id=(to_slab, target), device_id_type=MESH)

    for exists, to_slab in ((sends_far, far_out), (takes_far, far_in)):

        @pl.when(exists)
        def _():
            for step in range(n_sub):
                greet(barrier, to_slab, lax.rem(sub + step, n_sub))

    for step in range(n_sub):
        greet(barrier, kept, lax.rem(sub + step, n_sub))
    for step in range(1, n_sub):
        greet(barrier, slab, lax.rem(sub + step, n_sub))

    fars = sends_far.astype(jnp.int32) + takes_far.astype(jnp.int32)
    rounds = hello.shape[0]

    def pass_on(r):
        if r > 0:
            pl.semaphore_wait(hello.at[r - 1], fars)
        if r < rounds:
            pl.when(sends_far)(lambda: greet(hello.at[r], far_out, sub))
            pl.when(takes_far)(lambda: greet(hello.at[r], far_in, sub))

    n_used = tiles * coupled * halves
    if n_terms > n_used:
        terms[n_used:] = jnp.zeros((n_terms - n_used, LANES), f32)
        squares[n_used:] = jnp.zeros((n_terms - n_used, LANES), f32)

    @pl.when(jnp.logical_not(takes_far))
    def _():
        for ref in (first_in, *part_in):
            ref[2 * n_sub :] = jnp.zeros((n_sub,) + ref.shape[1:], f32)

    @pl.when(jnp.logical_not(sends_far))
    def _():
        blank = pl.ds(pl.multiple_of(far_rel * n_sub * held, 8), n_sub * held)
        for ref in field_in:
            ref[blank, :] = jnp.zeros((n_sub * held, LANES), f32)

    for copy in small:
        copy.wait()

    base = (slab - 1) * n_sub * NB_DEV
    lane = lax.broadcasted_iota(jnp.int32, (1, n_terms), 1)
    lane_tile = lane % tiles
    lane_k = lane // (halves * tiles)
    lane_h = (lane // tiles) % halves
    place = jnp.full((1, n_terms), -1, jnp.int32)
    for t in range(tiles):
        for k in range(coupled):
            at = jnp.clip((ids_smem[k, t] - base) * halves, 0, window - halves)
            wid[t, k] = at
            place = jnp.where(jnp.logical_and(lane_tile == t, lane_k == k), at + lane_h, place)
    selector[...] = (
        lax.broadcasted_iota(jnp.int32, (window, n_terms), 0) == place
    ).astype(f32).astype(jnp.bfloat16)

    def live(t):
        return jnp.where(t < counts_smem[0, 0], 1.0, 0.0).astype(f32)

    eye = (
        lax.broadcasted_iota(jnp.int32, (rows, LANES), 0)
        == lax.broadcasted_iota(jnp.int32, (rows, LANES), 1)
    ).astype(f32)

    def half(h):
        return slice(h * LANES, (h + 1) * LANES)

    def term_row(k, h, t):
        return pl.ds((k * halves + h) * tiles + t, 1)

    @pl.loop(0, tiles // group)
    def _(g):
        for i in range(group):
            t = g * group + i
            alive = right_ref[pl.ds(t, 1), :] * live(t)
            residual_ref[pl.ds(t, 1), :] = alive
            cols[t] = jnp.broadcast_to(
                jnp.sum(eye * alive, axis=1, keepdims=True), (rows, LANES)
            )

    def scatter(ref):
        full = ref[...]
        high = full.astype(jnp.bfloat16)
        low = (full - high.astype(f32)).astype(jnp.bfloat16)
        spread = jnp.dot(
            selector[...], jnp.concatenate([high, low], axis=1), preferred_element_type=f32
        )
        return (spread[:, :LANES] + spread[:, LANES:]).reshape(3 * pairs, span, LANES)

    def remote(src, dst, send, recv, device):
        return pltpu.make_async_remote_copy(
            src_ref=src, dst_ref=dst, send_sem=send, recv_sem=recv, device_id=device, device_id_type=MESH
        )

    def part_start(out_ref, in_ref, send, recv):
        def one(pos, rel, to_slab, step):
            target = lax.rem(pair + step, pairs)
            remote(
                out_ref.at[rel * pairs + target],
                in_ref.at[pos * n_sub + sub],
                send.at[pos // 2],
                recv.at[pos // 2],
                (to_slab, 2 * target + 1),
            ).start()

        @pl.when(sends_far)
        def _():
            for step in range(1, pairs + 1):
                one(2, far_rel, far_out, step)

        for step in range(1, pairs + 1):
            one(0, 1, kept, step)
        for step in range(1, pairs):
            one(1, own_rel, slab, step)
        pl.when(rests_here)(lambda: one(1, own_rel, slab, pairs))

        @pl.when(sums_here)
        def _():
            in_ref[n_sub + sub] = out_ref[own_rel * pairs + pair]

    def field_start(src, in_ref, send, recv):
        def one(sem, rel, to_slab, step, core):
            target = 2 * lax.rem(pair + step, pairs) + core
            at = pl.multiple_of((rel * pairs + pair) * span, 8)
            remote(
                src, in_ref.at[pl.ds(at, span)], send.at[sem], recv.at[sem], (to_slab, target)
            ).start()

        order = [(step, core) for core in range(2) for step in range(1, pairs + 1)]

        @pl.when(takes_far)
        def _():
            for step, core in order:
                one(1, kept - far_in + 1, far_in, step, core)

        for step, core in order:
            one(0, 1, kept, step, core)
        for step, core in order:
            if (step, core) != (pairs, 1):
                one(0, own_rel, slab, step, core)

    def group_wait(ref, per, sem, counts, far_too, recv):
        def wait(i, count):
            size = ref.at[pl.ds(0, count * per)]
            copy = remote(size, size, sem.at[i], sem.at[i], (kept, sub))
            copy.wait_recv() if recv else copy.wait_send()

        near, far = counts
        if isinstance(near, tuple):
            pl.when(sums_here)(lambda: wait(0, near[0]))
            pl.when(rests_here)(lambda: wait(0, near[1]))
        else:
            wait(0, near)
        pl.when(far_too)(lambda: wait(1, far))

    by_pair = ((2 * pairs - 1, 2 * pairs), pairs)
    by_sub = (2 * n_sub - 1, n_sub)

    summing = slab * pairs + pair

    def from_all(it):
        return it >= ITERS - 1

    def scal_copy(it, j):
        row = scal.at[it, pl.ds(me if from_all(it) else summing, 1)]
        return remote(row, row, scal_send.at[it], scal_recv.at[it], other(j))

    def scal_start(it, row):
        scal[it, pl.ds(me if from_all(it) else summing, 1)] = row

        @pl.loop(1, n, unroll=min(n - 1, 31))
        def _(j):
            scal_copy(it, j).start()

    def scal_wait(it, count, recv):
        rest = scal.at[it, pl.ds(0, count)]
        copy = remote(rest, rest, scal_send.at[it], scal_recv.at[it], other(1))
        copy.wait_recv() if recv else copy.wait_send()

    def scal_take(it):
        if from_all(it):
            scal_wait(it, n - 1, True)
        else:
            pl.when(sums_here)(lambda: scal_wait(it, n // 2 - 1, True))
            pl.when(rests_here)(lambda: scal_wait(it, n // 2, True))

    def total(x):
        return jnp.sum(jnp.sum(x, axis=0, keepdims=True), axis=1, keepdims=True)

    lane_row = lax.broadcasted_iota(jnp.int32, (1, LANES), 1)

    def pack(parts):
        row = jnp.zeros((1, LANES), f32)
        for i, x in enumerate(parts):
            row = jnp.where(lane_row == i, total(x), row)
        return row

    def unpack(it, count):
        row = jnp.sum(scal[it][: n if from_all(it) else n // 2], axis=0, keepdims=True)
        return [
            jnp.sum(jnp.where(lane_row == i, row, 0.0), axis=1, keepdims=True)
            for i in range(count)
        ]

    def turn(x):
        rest = jnp.zeros((LANES - tiles, LANES), f32)
        return jnp.concatenate([x, rest], axis=0).T

    @pl.loop(0, loads)
    def _(g):
        load(g).wait()
        for i in range(group):
            t = g * group + i
            alive = live(t)
            right = cols[t]
            for k in range(coupled):
                for h in range(halves):
                    a = values[t, k, :, half(h)]
                    terms[term_row(k, h, t), :] = jnp.sum(a * right, axis=0, keepdims=True)
                    squares[term_row(k, h, t), :] = (
                        jnp.sum(a * a, axis=0, keepdims=True) * alive
                    )

    for i, ref in enumerate((terms, squares)):
        first_out[:, i] = scatter(ref)
    pl.semaphore_wait(barrier, 2 * n_sub - 1 + n_sub * fars)
    part_start(first_out, first_in, first_send, first_recv)
    pass_on(0)
    pass_on(1)
    def own_rows(ref):
        return ref[pl.ds(pl.multiple_of((n_sub + sub) * held, 8), held), :]

    def send_field(it, field):
        field_out[it] = field
        at = pl.multiple_of((own_rel * pairs + pair) * span, 8)
        field_start(field_out.at[it], field_in[it], field_send.at[it], field_recv.at[it])
        field_in[it][pl.ds(at, span), :] = field

    @pl.when(sums_here)
    def _():
        group_wait(first_in, 1, first_recv, by_sub, takes_far, True)
        sums = jnp.sum(first_in[...], axis=0)
        jacobi[...] = 1.0 / (1.0 + sums[1])
        scaled[...] = jacobi[...] * sums[0]
        kept_dir[...] = scaled[...]
        send_field(0, scaled[...])
        rho_row[...] = jnp.where(lane_row == SUMS, total(sums[0] * scaled[...]), 0.0)

    answer = jnp.zeros((held, LANES), f32)
    for it in range(ITERS):
        last = it == ITERS - 1
        fields = field_in[it]
        group_wait(fields, span, field_recv.at[it], by_pair, sends_far, True)

        def reduced(t):
            alive = live(t)
            m = None
            for k in range(coupled):
                for h in range(halves):
                    picked = fields[pl.ds(wid[t, k] + h, 1), :] * alive
                    product = values[t, k, :, half(h)] * picked
                    m = product if m is None else m + product
            return jnp.broadcast_to(jnp.sum(m, axis=1, keepdims=True), (rows, LANES))

        def forward(t):
            cols[t] = reduced(t)

        def backward(t):
            image = cols[t]
            for k in range(coupled):
                for h in range(halves):
                    terms[term_row(k, h, t), :] = jnp.sum(
                        values[t, k, :, half(h)] * image, axis=0, keepdims=True
                    )

        step = divisor(tiles, STEP, 3, 2)
        if last:

            def turned_step(g, turned):
                for i in range(step):
                    t = g * step + i
                    turned = jnp.where(lane_row == t, reduced(t), turned)
                return turned

            image_t = turn(image)
            turned = turn(scaled_image)
            pushed = lax.fori_loop(0, tiles // step, turned_step, jnp.zeros((rows, LANES), f32))
        else:
            for i in range(step):
                forward(i)

            @pl.loop(1, tiles // step)
            def _(g):
                for i in range(step):
                    backward((g - 1) * step + i)
                for i in range(step):
                    forward(g * step + i)

            for i in range(step):
                backward(tiles - step + i)
            part_out[it] = scatter(terms)
            part_start(part_out.at[it], part_in[it], part_send.at[it], part_recv.at[it])

            @pl.loop(0, tiles, unroll=4)
            def _(t):
                rows_ref[pl.ds(t, 1), :] = jnp.sum(cols[t] * eye, axis=0, keepdims=True)

        field_own = own_rows(fields)
        if it == 0:
            for r in range(2, rounds + 1):
                pass_on(r)
            scaled_own = field_own
            direction = field_own
            scaled_image = rows_ref[...]
            image = scaled_image
        elif last:
            scal_take(ITERS)
            curve, cross = unpack(ITERS, 2)
            step_size = rho / curve
            turned = turned - step_size * pushed
            scal_start(
                it, pack((turned * turned, turned * image_t, image_t * image_t))
            )
            answer = answer + step_size * direction
            residual = residual_ref[...] - step_size * image
            scaled_own = scaled_own - step_size * field_own
            scaled_image = turned.T[:tiles]
            scal_take(it - 1)
            (square,) = unpack(it - 1, 1)
            rho_next = rho - 2.0 * step_size * cross + step_size * step_size * square
            beta = rho_next / rho
            rho = rho_next
            direction = scaled_own + beta * direction
            image = scaled_image + beta * image
        else:
            scal_take(it - 1)
            if it == 1:
                curve, cross, square, rho = unpack(it - 1, SUMS + 1)
            else:
                curve, cross, square = unpack(it - 1, SUMS)
            step_size = rho / curve
            rho_next = rho - 2.0 * step_size * cross + step_size * step_size * square
            beta = rho_next / rho
            rho = rho_next
            answer = answer + step_size * direction
            residual_ref[...] = residual_ref[...] - step_size * image
            scaled_own = scaled_own - step_size * field_own
            direction = scaled_own + beta * direction
            scaled_image = scaled_image - step_size * rows_ref[...]
            image = scaled_image + beta * image

        if it == ITERS - 2:
            scal_start(ITERS, pack((image * image, scaled_image * image)))
        if not last:

            @pl.when(sums_here)
            def _():
                if it > 0:
                    scaled[...] = scaled[...] - step_size * field_out[it]
                    kept_dir[...] = scaled[...] + beta * kept_dir[...]
                group_wait(part_in[it], 1, part_recv.at[it], by_sub, takes_far, True)
                spread = jnp.sum(part_in[it][...], axis=0)
                if it == 0:
                    scaled_back[...] = spread
                    back[...] = spread
                else:
                    scaled_back[...] = scaled_back[...] - step_size * spread
                    back[...] = scaled_back[...] + beta * back[...]
                field = jacobi[...] * back[...]
                send_field(it + 1, field)
                square = back[...] * field
                if it == ITERS - 2:
                    row = pack((square,))
                else:
                    row = pack((kept_dir[...] * back[...], scaled[...] * back[...], square))
                scal_start(it, row + rho_row[...] if it == 0 else row)

    scal_take(ITERS - 1)
    new, mixed, old = unpack(ITERS - 1, SUMS)
    step_size = rho / (new + 2.0 * beta * mixed + beta * beta * old)
    answer = answer + step_size * direction
    residual_ref[...] = residual - step_size * image
    rows_ref[:held] = answer
    for h in range(halves):
        solution_ref[:, half(h)] = rows_ref[pl.ds(h, NB_DEV, stride=halves), :]

    group_wait(first_in, 1, first_send, by_pair, sends_far, False)
    for it in range(ITERS - 1):
        group_wait(part_in[it], 1, part_send.at[it], by_pair, sends_far, False)
    for it in (ITERS - 1, ITERS):
        scal_wait(it, n - 1, False)

    @pl.when(sums_here)
    def _():
        for it in range(ITERS):
            group_wait(part_in[0], 1, field_send.at[it], by_sub, takes_far, False)
        for it in range(ITERS - 1):
            scal_wait(it, n - 1, False)


def per_device(n_slab, n_sub, values, block_ids, tile_counts, right_side):
    tiles, coupled, rows, block = values.shape
    halves = block // LANES
    held = NB_DEV * halves
    n = n_slab * n_sub
    slots = 3 * n_sub
    window = slots * held
    span = 2 * held
    pairs = n_sub // 2
    n_terms = round_up(tiles * coupled * halves, LANES)
    loads = tiles // divisor(tiles, 4, 3, 2)
    f32 = jnp.float32
    vmem = pltpu.VMEM
    dma = pltpu.SemaphoreType.DMA
    whole = pl.BlockSpec(memory_space=pltpu.VMEM)
    return pl.pallas_call(
        functools.partial(kernel, n_slab, n_sub),
        out_shape=(
            jax.ShapeDtypeStruct((NB_DEV, block), f32),
            jax.ShapeDtypeStruct((tiles, rows), f32),
        ),
        in_specs=[pl.BlockSpec(memory_space=pltpu.HBM)] * 4,
        out_specs=(whole, whole),
        scratch_shapes=[
            vmem(values.shape, f32),
            pltpu.SMEM((tiles, coupled), jnp.int32),
            vmem((window, n_terms), jnp.bfloat16),
            vmem((n_terms, LANES), f32),
            vmem((n_terms, LANES), f32),
            vmem((tiles, rows, LANES), f32),
            vmem((tiles, LANES), f32),
            vmem((3 * pairs, 2, span, LANES), f32),
            vmem((slots, 2, span, LANES), f32),
            vmem((ITERS - 1, 3 * pairs, span, LANES), f32),
            [vmem((slots, span, LANES), f32)] * (ITERS - 1),
            vmem((ITERS, span, LANES), f32),
            [vmem((window, LANES), f32)] * ITERS,
            vmem((ITERS + 1, n, LANES), f32),
            pltpu.SMEM((coupled, tiles), jnp.int32),
            pltpu.SMEM((1, 1), jnp.int32),
            vmem((tiles, rows), f32),
            dma((3,)),
            dma((loads,)),
            dma((2,)),
            dma((2,)),
            dma((ITERS - 1, 2)),
            dma((ITERS - 1, 2)),
            dma((ITERS, 2)),
            dma((ITERS, 2)),
            dma((ITERS + 1,)),
            dma((ITERS + 1,)),
            pltpu.SemaphoreType.REGULAR((max(1, n_slab // 2 - 1),)),
            *([vmem((span, LANES), f32)] * 5),
            vmem((1, LANES), f32),
        ],
        compiler_params=pltpu.CompilerParams(
            collective_id=0, has_side_effects=True, vmem_limit_bytes=48 * 1024 * 1024
        ),
    )(values, block_ids.T, tile_counts, right_side)


def solution(mesh):
    in_specs = (
        P(("slab", "sub"), None, None, None),
        P(("slab", "sub"), None),
        P("slab", "sub"),
        P(("slab", "sub"), None),
    )
    out_specs = (P(("slab", "sub"), None), P(("slab", "sub"), None))
    return jax.shard_map(
        functools.partial(per_device, mesh.shape["slab"], mesh.shape["sub"]),
        mesh=mesh,
        in_specs=in_specs,
        out_specs=out_specs,
        check_vma=False,
    )
```

```python
import functools

import jax
import jax.numpy as jnp
from jax import lax
from jax.experimental import pallas as pl
from jax.experimental.pallas import tpu as pltpu
from jax.sharding import PartitionSpec as P

ITERS = 4
NB_DEV = 12
LANES = 128
SUMS = 3
STEP = 12
ORDER = 2
AHEAD = 4
GROUP = 4
SUBLANES = 8
MESH = pl.DeviceIdType.MESH


def round_up(size, unit):
    return -(-size // unit) * unit


def divisor(size, *wanted):
    return next(g for g in (*wanted, 1) if size % g == 0)


def kernel(
    n_slab,
    n_sub,
    values_hbm,
    ids_hbm,
    counts_hbm,
    right_hbm,
    solution_ref,
    residual_ref,
    values,
    wid,
    selector,
    terms,
    squares,
    cols,
    rows_ref,
    first_out,
    first_in,
    part_out,
    part_in,
    field_out,
    field_in,
    scal,
    ids_smem,
    counts_smem,
    right_ref,
    small_sem,
    load_sem,
    first_send,
    first_recv,
    part_send,
    part_recv,
    field_send,
    field_recv,
    scal_send,
    scal_recv,
    hello,
    jacobi,
    scaled,
    kept_dir,
    scaled_back,
    back,
    rho_row,
):
    tiles, coupled, rows, block = values.shape
    halves = block // LANES
    held = NB_DEV * halves
    n = n_slab * n_sub
    window = 3 * n_sub * held
    n_terms = terms.shape[0]
    f32 = jnp.float32
    slab = lax.axis_index("slab")
    sub = lax.axis_index("sub")
    me = slab * n_sub + sub
    pairs = n_sub // 2
    span = 2 * held
    pair = lax.div(sub, 2)
    sums_here = lax.rem(sub, 2) == 1
    rests_here = lax.rem(sub, 2) == 0

    kept = slab + 1 - 2 * lax.rem(slab, 2)
    own_rel = kept - slab + 1
    beyond = 2 * slab - kept
    far_rel = slab - kept + 1
    far_out = 3 * slab - 2 * kept
    far_in = 2 * kept - slab
    sends_far = jnp.logical_and(beyond >= 0, beyond < n_slab)
    takes_far = jnp.logical_and(far_in >= 0, far_in < n_slab)

    small = [
        pltpu.make_async_copy(src, dst, small_sem.at[i])
        for i, (src, dst) in enumerate(
            ((ids_hbm, ids_smem), (counts_hbm, counts_smem), (right_hbm, right_ref))
        )
    ]
    for copy in small:
        copy.start()
    loads = load_sem.shape[0]
    group = tiles // loads

    def load(g):
        part = pl.ds(g * group, group)
        return pltpu.make_async_copy(values_hbm.at[part], values.at[part], load_sem.at[g])

    ahead = min(AHEAD, loads)
    for g in range(ahead):
        load(g).start()

    def other(j):
        target = lax.rem(me + j, n)
        return (lax.div(target, n_sub), lax.rem(target, n_sub))

    barrier = pltpu.get_barrier_semaphore()

    def greet(slot, to_slab, target):
        pl.semaphore_signal(slot, inc=1, device_id=(to_slab, target), device_id_type=MESH)

    for exists, to_slab in ((sends_far, far_out), (takes_far, far_in)):

        @pl.when(exists)
        def _():
            for step in range(n_sub):
                greet(barrier, to_slab, lax.rem(sub + step, n_sub))

    for step in range(n_sub):
        greet(barrier, kept, lax.rem(sub + step, n_sub))
    for step in range(1, n_sub):
        greet(barrier, slab, lax.rem(sub + step, n_sub))

    fars = sends_far.astype(jnp.int32) + takes_far.astype(jnp.int32)
    rounds = hello.shape[0]

    def pass_on(r):
        if r > 0:
            pl.semaphore_wait(hello.at[r - 1], fars)
        if r < rounds:
            pl.when(sends_far)(lambda: greet(hello.at[r], far_out, sub))
            pl.when(takes_far)(lambda: greet(hello.at[r], far_in, sub))

    n_used = tiles * coupled * halves
    if n_terms > n_used:
        terms[n_used:] = jnp.zeros((n_terms - n_used, LANES), f32)
        squares[n_used:] = jnp.zeros((n_terms - n_used, LANES), f32)

    @pl.when(jnp.logical_not(takes_far))
    def _():
        for ref in (first_in, *part_in):
            ref[2 * n_sub :] = jnp.zeros((n_sub,) + ref.shape[1:], f32)

    @pl.when(jnp.logical_not(sends_far))
    def _():
        blank = pl.ds(pl.multiple_of(far_rel * n_sub * held, 8), n_sub * held)
        for ref in field_in:
            ref[blank, :] = jnp.zeros((n_sub * held, LANES), f32)

    for copy in small:
        copy.wait()

    base = (slab - 1) * n_sub * NB_DEV
    lane = lax.broadcasted_iota(jnp.int32, (1, n_terms), 1)
    lane_tile = lane % tiles
    lane_k = lane // (halves * tiles)
    lane_h = (lane // tiles) % halves
    place = jnp.full((1, n_terms), -1, jnp.int32)
    for t in range(tiles):
        for k in range(coupled):
            at = jnp.clip((ids_smem[k, t] - base) * halves, 0, window - halves)
            wid[t, k] = at
            place = jnp.where(jnp.logical_and(lane_tile == t, lane_k == k), at + lane_h, place)
    selector[...] = (
        lax.broadcasted_iota(jnp.int32, (window, n_terms), 0) == place
    ).astype(f32).astype(jnp.bfloat16)

    def live(t):
        return jnp.where(t < counts_smem[0, 0], 1.0, 0.0).astype(f32)

    eye = (
        lax.broadcasted_iota(jnp.int32, (rows, LANES), 0)
        == lax.broadcasted_iota(jnp.int32, (rows, LANES), 1)
    ).astype(f32)

    def half(h):
        return slice(h * LANES, (h + 1) * LANES)

    bands = rows // SUBLANES

    def band(r):
        return pl.ds(r * SUBLANES, SUBLANES)

    def term_row(k, h, t):
        return pl.ds((k * halves + h) * tiles + t, 1)

    def spread_right(g):
        for i in range(group):
            t = g * group + i
            row = right_ref[pl.ds(t, 1), :] * live(t)
            residual_ref[pl.ds(t, 1), :] = row
            for r in range(bands):
                cols[t, band(r), :] = jnp.broadcast_to(
                    jnp.sum(eye[r * SUBLANES : (r + 1) * SUBLANES] * row, axis=1, keepdims=True),
                    (SUBLANES, LANES),
                )

    spread_right(0)

    def scatter(ref):
        full = ref[...]
        high = full.astype(jnp.bfloat16)
        low = (full - high.astype(f32)).astype(jnp.bfloat16)
        spread = jnp.dot(
            selector[...], jnp.concatenate([high, low], axis=1), preferred_element_type=f32
        )
        return (spread[:, :LANES] + spread[:, LANES:]).reshape(3 * pairs, span, LANES)

    def remote(src, dst, send, recv, device):
        return pltpu.make_async_remote_copy(
            src_ref=src, dst_ref=dst, send_sem=send, recv_sem=recv, device_id=device, device_id_type=MESH
        )

    def part_start(out_ref, in_ref, send, recv):
        def one(pos, rel, to_slab, step):
            target = lax.rem(pair + step, pairs)
            remote(
                out_ref.at[rel * pairs + target],
                in_ref.at[pos * n_sub + sub],
                send.at[pos // 2],
                recv.at[pos // 2],
                (to_slab, 2 * target + 1),
            ).start()

        @pl.when(sends_far)
        def _():
            for step in range(1, pairs + 1):
                one(2, far_rel, far_out, step)

        for step in range(1, pairs + 1):
            one(0, 1, kept, step)
        for step in range(1, pairs):
            one(1, own_rel, slab, step)
        pl.when(rests_here)(lambda: one(1, own_rel, slab, pairs))

        @pl.when(sums_here)
        def _():
            in_ref[n_sub + sub] = out_ref[own_rel * pairs + pair]

    def field_start(src, in_ref, send, recv):
        def one(sem, rel, to_slab, step, core):
            target = 2 * lax.rem(pair + step, pairs) + core
            at = pl.multiple_of((rel * pairs + pair) * span, 8)
            remote(
                src, in_ref.at[pl.ds(at, span)], send.at[sem], recv.at[sem], (to_slab, target)
            ).start()

        order = [(step, core) for core in range(2) for step in range(1, pairs + 1)]

        @pl.when(takes_far)
        def _():
            for step, core in order:
                one(1, kept - far_in + 1, far_in, step, core)

        for step, core in order:
            one(0, 1, kept, step, core)
        for step, core in order:
            if (step, core) != (pairs, 1):
                one(0, own_rel, slab, step, core)

    def group_wait(ref, per, sem, counts, far_too, recv):
        def wait(i, count):
            size = ref.at[pl.ds(0, count * per)]
            copy = remote(size, size, sem.at[i], sem.at[i], (kept, sub))
            copy.wait_recv() if recv else copy.wait_send()

        near, far = counts
        if isinstance(near, tuple):
            pl.when(sums_here)(lambda: wait(0, near[0]))
            pl.when(rests_here)(lambda: wait(0, near[1]))
        else:
            wait(0, near)
        pl.when(far_too)(lambda: wait(1, far))

    by_pair = ((2 * pairs - 1, 2 * pairs), pairs)
    by_sub = (2 * n_sub - 1, n_sub)

    summing = slab * pairs + pair

    def from_all(it):
        return it >= ITERS - 1

    def scal_copy(it, j):
        row = scal.at[it, pl.ds(me if from_all(it) else summing, 1)]
        return remote(row, row, scal_send.at[it], scal_recv.at[it], other(j))

    def scal_start(it, row):
        scal[it, pl.ds(me if from_all(it) else summing, 1)] = row

        @pl.loop(1, n, unroll=min(n - 1, 31))
        def _(j):
            scal_copy(it, j).start()

    def scal_wait(it, count, recv):
        rest = scal.at[it, pl.ds(0, count)]
        copy = remote(rest, rest, scal_send.at[it], scal_recv.at[it], other(1))
        copy.wait_recv() if recv else copy.wait_send()

    def scal_take(it):
        if from_all(it):
            scal_wait(it, n - 1, True)
        else:
            pl.when(sums_here)(lambda: scal_wait(it, n // 2 - 1, True))
            pl.when(rests_here)(lambda: scal_wait(it, n // 2, True))

    def total(x):
        return jnp.sum(jnp.sum(x, axis=0, keepdims=True), axis=1, keepdims=True)

    lane_row = lax.broadcasted_iota(jnp.int32, (1, LANES), 1)

    def pack(parts):
        row = jnp.zeros((1, LANES), f32)
        for i, x in enumerate(parts):
            row = jnp.where(lane_row == i, total(x), row)
        return row

    def unpack(it, count):
        row = jnp.sum(scal[it][: n if from_all(it) else n // 2], axis=0, keepdims=True)
        return [
            jnp.sum(jnp.where(lane_row == i, row, 0.0), axis=1, keepdims=True)
            for i in range(count)
        ]

    def turn(x):
        rest = jnp.zeros((LANES - tiles, LANES), f32)
        return jnp.concatenate([x, rest], axis=0).T

    @pl.loop(0, loads)
    def _(g):
        load(g).wait()
        pl.when(g + ahead < loads)(lambda: load(g + ahead).start())
        for i in range(group):
            t = g * group + i
            alive = live(t)
            n_sums = coupled * halves
            sums = [None] * (2 * n_sums)
            for r in range(bands):
                right = cols[t, band(r), :]
                for k in range(coupled):
                    for h in range(halves):
                        j = k * halves + h
                        a = values[t, k, band(r), half(h)]
                        sums[j] = a * right if r == 0 else sums[j] + a * right
                        sums[n_sums + j] = a * a if r == 0 else sums[n_sums + j] + a * a
            for k in range(coupled):
                for h in range(halves):
                    j = k * halves + h
                    terms[term_row(k, h, t), :] = jnp.sum(sums[j], axis=0, keepdims=True)
                    squares[term_row(k, h, t), :] = (
                        jnp.sum(sums[n_sums + j], axis=0, keepdims=True) * alive
                    )
        spread_right(jnp.minimum(g + 1, loads - 1))

    for i, ref in enumerate((terms, squares)):
        first_out[:, i] = scatter(ref)
    pl.semaphore_wait(barrier, 2 * n_sub - 1 + n_sub * fars)
    part_start(first_out, first_in, first_send, first_recv)
    pass_on(0)
    pass_on(1)
    def own_rows(ref):
        return ref[pl.ds(pl.multiple_of((n_sub + sub) * held, 8), held), :]

    def send_field(it, field):
        field_out[it] = field
        at = pl.multiple_of((own_rel * pairs + pair) * span, 8)
        field_start(field_out.at[it], field_in[it], field_send.at[it], field_recv.at[it])
        field_in[it][pl.ds(at, span), :] = field

    @pl.when(sums_here)
    def _():
        group_wait(first_in, 1, first_recv, by_sub, takes_far, True)
        sums = jnp.sum(first_in[...], axis=0)
        jacobi[...] = 1.0 / (1.0 + sums[1])
        scaled[...] = jacobi[...] * sums[0]
        kept_dir[...] = scaled[...]
        send_field(0, scaled[...])
        rho_row[...] = jnp.where(lane_row == SUMS, total(sums[0] * scaled[...]), 0.0)

    answer = jnp.zeros((held, LANES), f32)
    for it in range(ITERS):
        last = it == ITERS - 1
        fields = field_in[it]
        group_wait(fields, span, field_recv.at[it], by_pair, sends_far, True)

        def picked(t):
            alive = live(t)
            return [
                jnp.broadcast_to(
                    fields[pl.ds(wid[t, k] + h, 1), :] * alive, (SUBLANES, LANES)
                )
                for k in range(coupled)
                for h in range(halves)
            ]

        def reduced(t, r, row):
            m = None
            for k in range(coupled):
                for h in range(halves):
                    product = values[t, k, band(r), half(h)] * row[k * halves + h]
                    m = product if m is None else m + product
            return jnp.broadcast_to(jnp.sum(m, axis=1, keepdims=True), (SUBLANES, LANES))

        def forward(t):
            row = picked(t)
            for r in range(bands):
                cols[t, band(r), :] = reduced(t, r, row)

        def backward(t):
            sums = [None] * (coupled * halves)
            for r in range(bands):
                image = cols[t, band(r), :]
                for k in range(coupled):
                    for h in range(halves):
                        i = k * halves + h
                        product = values[t, k, band(r), half(h)] * image
                        sums[i] = product if r == 0 else sums[i] + product
            for k in range(coupled):
                for h in range(halves):
                    terms[term_row(k, h, t), :] = jnp.sum(
                        sums[k * halves + h], axis=0, keepdims=True
                    )

        step = divisor(tiles, STEP, 3, 2)
        if last:

            def turned_step(g, turned):
                for i in range(step):
                    t = g * step + i
                    row = picked(t)
                    here = lane_row == t
                    turned = [
                        jnp.where(here, reduced(t, r, row), turned[r]) for r in range(bands)
                    ]
                return turned

            image_t = turn(image)
            turned = turn(scaled_image)
            pushed = jnp.concatenate(
                lax.fori_loop(
                    0,
                    tiles // step,
                    turned_step,
                    [jnp.zeros((SUBLANES, LANES), f32)] * bands,
                ),
                axis=0,
            )
        else:
            if ORDER == 2:

                @pl.loop(0, tiles // step)
                def _(g):
                    for i in range(step):
                        forward(g * step + i)

                @pl.loop(0, tiles // step)
                def _(g):
                    for i in range(step):
                        backward(g * step + i)

            else:
                for i in range(step):
                    forward(i)

                @pl.loop(1, tiles // step)
                def _(g):
                    for i in range(step):
                        if ORDER == 0:
                            backward((g - 1) * step + i)
                        else:
                            forward(g * step + i)
                    for i in range(step):
                        if ORDER == 1:
                            backward((g - 1) * step + i)
                        else:
                            forward(g * step + i)

                for i in range(step):
                    backward(tiles - step + i)
            part_out[it] = scatter(terms)
            part_start(part_out.at[it], part_in[it], part_send.at[it], part_recv.at[it])

            @pl.loop(0, tiles, unroll=4)
            def _(t):
                rows_ref[pl.ds(t, 1), :] = jnp.sum(cols[t] * eye, axis=0, keepdims=True)

        field_own = own_rows(fields)
        if it == 0:
            for r in range(2, rounds + 1):
                pass_on(r)
            scaled_own = field_own
            direction = field_own
            scaled_image = rows_ref[...]
            image = scaled_image
        elif last:
            scal_take(ITERS)
            curve, cross = unpack(ITERS, 2)
            step_size = rho / curve
            turned = turned - step_size * pushed
            scal_start(
                it, pack((turned * turned, turned * image_t, image_t * image_t))
            )
            answer = answer + step_size * direction
            residual = residual_ref[...] - step_size * image
            scaled_own = scaled_own - step_size * field_own
            scaled_image = turned.T[:tiles]
            scal_take(it - 1)
            (square,) = unpack(it - 1, 1)
            rho_next = rho - 2.0 * step_size * cross + step_size * step_size * square
            beta = rho_next / rho
            rho = rho_next
            direction = scaled_own + beta * direction
            image = scaled_image + beta * image
        else:
            scal_take(it - 1)
            if it == 1:
                curve, cross, square, rho = unpack(it - 1, SUMS + 1)
            else:
                curve, cross, square = unpack(it - 1, SUMS)
            step_size = rho / curve
            rho_next = rho - 2.0 * step_size * cross + step_size * step_size * square
            beta = rho_next / rho
            rho = rho_next
            answer = answer + step_size * direction
            residual_ref[...] = residual_ref[...] - step_size * image
            scaled_own = scaled_own - step_size * field_own
            direction = scaled_own + beta * direction
            scaled_image = scaled_image - step_size * rows_ref[...]
            image = scaled_image + beta * image

        if it == ITERS - 2:
            scal_start(ITERS, pack((image * image, scaled_image * image)))
        if not last:

            @pl.when(sums_here)
            def _():
                if it > 0:
                    scaled[...] = scaled[...] - step_size * field_out[it]
                    kept_dir[...] = scaled[...] + beta * kept_dir[...]
                group_wait(part_in[it], 1, part_recv.at[it], by_sub, takes_far, True)
                spread = jnp.sum(part_in[it][...], axis=0)
                if it == 0:
                    scaled_back[...] = spread
                    back[...] = spread
                else:
                    scaled_back[...] = scaled_back[...] - step_size * spread
                    back[...] = scaled_back[...] + beta * back[...]
                field = jacobi[...] * back[...]
                send_field(it + 1, field)
                square = back[...] * field
                if it == ITERS - 2:
                    row = pack((square,))
                else:
                    row = pack((kept_dir[...] * back[...], scaled[...] * back[...], square))
                scal_start(it, row + rho_row[...] if it == 0 else row)

    scal_take(ITERS - 1)
    new, mixed, old = unpack(ITERS - 1, SUMS)
    step_size = rho / (new + 2.0 * beta * mixed + beta * beta * old)
    answer = answer + step_size * direction
    residual_ref[...] = residual - step_size * image
    rows_ref[:held] = answer
    for h in range(halves):
        solution_ref[:, half(h)] = rows_ref[pl.ds(h, NB_DEV, stride=halves), :]

    group_wait(first_in, 1, first_send, by_pair, sends_far, False)
    for it in range(ITERS - 1):
        group_wait(part_in[it], 1, part_send.at[it], by_pair, sends_far, False)
    for it in (ITERS - 1, ITERS):
        scal_wait(it, n - 1, False)

    @pl.when(sums_here)
    def _():
        for it in range(ITERS):
            group_wait(part_in[0], 1, field_send.at[it], by_sub, takes_far, False)
        for it in range(ITERS - 1):
            scal_wait(it, n - 1, False)


def per_device(n_slab, n_sub, values, block_ids, tile_counts, right_side):
    tiles, coupled, rows, block = values.shape
    halves = block // LANES
    held = NB_DEV * halves
    n = n_slab * n_sub
    slots = 3 * n_sub
    window = slots * held
    span = 2 * held
    pairs = n_sub // 2
    n_terms = round_up(tiles * coupled * halves, LANES)
    loads = tiles // divisor(tiles, GROUP, 3, 2)
    f32 = jnp.float32
    vmem = pltpu.VMEM
    dma = pltpu.SemaphoreType.DMA
    whole = pl.BlockSpec(memory_space=pltpu.VMEM)
    return pl.pallas_call(
        functools.partial(kernel, n_slab, n_sub),
        out_shape=(
            jax.ShapeDtypeStruct((NB_DEV, block), f32),
            jax.ShapeDtypeStruct((tiles, rows), f32),
        ),
        in_specs=[pl.BlockSpec(memory_space=pltpu.HBM)] * 4,
        out_specs=(whole, whole),
        scratch_shapes=[
            vmem(values.shape, f32),
            pltpu.SMEM((tiles, coupled), jnp.int32),
            vmem((window, n_terms), jnp.bfloat16),
            vmem((n_terms, LANES), f32),
            vmem((n_terms, LANES), f32),
            vmem((tiles, rows, LANES), f32),
            vmem((tiles, LANES), f32),
            vmem((3 * pairs, 2, span, LANES), f32),
            vmem((slots, 2, span, LANES), f32),
            vmem((ITERS - 1, 3 * pairs, span, LANES), f32),
            [vmem((slots, span, LANES), f32)] * (ITERS - 1),
            vmem((ITERS, span, LANES), f32),
            [vmem((window, LANES), f32)] * ITERS,
            vmem((ITERS + 1, n, LANES), f32),
            pltpu.SMEM((coupled, tiles), jnp.int32),
            pltpu.SMEM((1, 1), jnp.int32),
            vmem((tiles, rows), f32),
            dma((3,)),
            dma((loads,)),
            dma((2,)),
            dma((2,)),
            dma((ITERS - 1, 2)),
            dma((ITERS - 1, 2)),
            dma((ITERS, 2)),
            dma((ITERS, 2)),
            dma((ITERS + 1,)),
            dma((ITERS + 1,)),
            pltpu.SemaphoreType.REGULAR((max(1, n_slab // 2 - 1),)),
            *([vmem((span, LANES), f32)] * 5),
            vmem((1, LANES), f32),
        ],
        compiler_params=pltpu.CompilerParams(
            collective_id=0, has_side_effects=True, vmem_limit_bytes=48 * 1024 * 1024
        ),
    )(values, pltpu.with_memory_space_constraint(block_ids.T, pltpu.HBM), tile_counts, pltpu.with_memory_space_constraint(right_side, pltpu.HBM))


def solution(mesh):
    in_specs = (
        P(("slab", "sub"), None, None, None),
        P(("slab", "sub"), None),
        P("slab", "sub"),
        P(("slab", "sub"), None),
    )
    out_specs = (P(("slab", "sub"), None), P(("slab", "sub"), None))
    return jax.shard_map(
        functools.partial(per_device, mesh.shape["slab"], mesh.shape["sub"]),
        mesh=mesh,
        in_specs=in_specs,
        out_specs=out_specs,
        check_vma=False,
    )
```

```python
import functools

import jax
import jax.numpy as jnp
from jax import lax
from jax.experimental import pallas as pl
from jax.experimental.pallas import tpu as pltpu
from jax.sharding import PartitionSpec as P

ITERS = 4
NB_DEV = 12
LANES = 128
SUMS = 3
STEP = 12
ORDER = 2
LAST = 24
AHEAD = 4
GROUP = 4
SUBLANES = 8
MESH = pl.DeviceIdType.MESH


def round_up(size, unit):
    return -(-size // unit) * unit


def divisor(size, *wanted):
    return next(g for g in (*wanted, 1) if size % g == 0)


def kernel(
    n_slab,
    n_sub,
    values_hbm,
    ids_hbm,
    counts_hbm,
    right_hbm,
    solution_ref,
    residual_ref,
    values,
    wid,
    selector,
    terms,
    squares,
    cols,
    rows_ref,
    first_out,
    first_in,
    part_out,
    part_in,
    field_out,
    field_in,
    scal,
    ids_smem,
    counts_smem,
    right_ref,
    small_sem,
    load_sem,
    first_send,
    first_recv,
    part_send,
    part_recv,
    field_send,
    field_recv,
    scal_send,
    scal_recv,
    hello,
    jacobi,
    scaled,
    kept_dir,
    scaled_back,
    back,
    rho_row,
):
    tiles, coupled, rows, block = values.shape
    halves = block // LANES
    held = NB_DEV * halves
    n = n_slab * n_sub
    window = 3 * n_sub * held
    n_terms = terms.shape[0]
    f32 = jnp.float32
    slab = lax.axis_index("slab")
    sub = lax.axis_index("sub")
    me = slab * n_sub + sub
    pairs = n_sub // 2
    span = 2 * held
    pair = lax.div(sub, 2)
    sums_here = lax.rem(sub, 2) == 1
    rests_here = lax.rem(sub, 2) == 0

    kept = slab + 1 - 2 * lax.rem(slab, 2)
    own_rel = kept - slab + 1
    beyond = 2 * slab - kept
    far_rel = slab - kept + 1
    far_out = 3 * slab - 2 * kept
    far_in = 2 * kept - slab
    sends_far = jnp.logical_and(beyond >= 0, beyond < n_slab)
    takes_far = jnp.logical_and(far_in >= 0, far_in < n_slab)

    small = [
        pltpu.make_async_copy(src, dst, small_sem.at[i])
        for i, (src, dst) in enumerate(
            ((ids_hbm, ids_smem), (counts_hbm, counts_smem), (right_hbm, right_ref))
        )
    ]
    for copy in small:
        copy.start()
    loads = load_sem.shape[0]
    group = tiles // loads

    def load(g):
        part = pl.ds(g * group, group)
        return pltpu.make_async_copy(values_hbm.at[part], values.at[part], load_sem.at[g])

    ahead = min(AHEAD, loads)
    for g in range(ahead):
        load(g).start()

    def other(j):
        target = lax.rem(me + j, n)
        return (lax.div(target, n_sub), lax.rem(target, n_sub))

    barrier = pltpu.get_barrier_semaphore()

    def greet(slot, to_slab, target):
        pl.semaphore_signal(slot, inc=1, device_id=(to_slab, target), device_id_type=MESH)

    for exists, to_slab in ((sends_far, far_out), (takes_far, far_in)):

        @pl.when(exists)
        def _():
            for step in range(n_sub):
                greet(barrier, to_slab, lax.rem(sub + step, n_sub))

    for step in range(n_sub):
        greet(barrier, kept, lax.rem(sub + step, n_sub))
    for step in range(1, n_sub):
        greet(barrier, slab, lax.rem(sub + step, n_sub))

    fars = sends_far.astype(jnp.int32) + takes_far.astype(jnp.int32)
    rounds = hello.shape[0]

    def pass_on(r):
        if r > 0:
            pl.semaphore_wait(hello.at[r - 1], fars)
        if r < rounds:
            pl.when(sends_far)(lambda: greet(hello.at[r], far_out, sub))
            pl.when(takes_far)(lambda: greet(hello.at[r], far_in, sub))

    n_used = tiles * coupled * halves
    if n_terms > n_used:
        terms[n_used:] = jnp.zeros((n_terms - n_used, LANES), f32)
        squares[n_used:] = jnp.zeros((n_terms - n_used, LANES), f32)

    @pl.when(jnp.logical_not(takes_far))
    def _():
        for ref in (first_in, *part_in):
            ref[2 * n_sub :] = jnp.zeros((n_sub,) + ref.shape[1:], f32)

    @pl.when(jnp.logical_not(sends_far))
    def _():
        blank = pl.ds(pl.multiple_of(far_rel * n_sub * held, 8), n_sub * held)
        for ref in field_in:
            ref[blank, :] = jnp.zeros((n_sub * held, LANES), f32)

    for copy in small:
        copy.wait()

    base = (slab - 1) * n_sub * NB_DEV
    lane = lax.broadcasted_iota(jnp.int32, (1, n_terms), 1)
    lane_tile = lane % tiles
    lane_k = lane // (halves * tiles)
    lane_h = (lane // tiles) % halves
    place = jnp.full((1, n_terms), -1, jnp.int32)
    for t in range(tiles):
        for k in range(coupled):
            at = jnp.clip((ids_smem[k, t] - base) * halves, 0, window - halves)
            wid[t, k] = at
            place = jnp.where(jnp.logical_and(lane_tile == t, lane_k == k), at + lane_h, place)
    selector[...] = (
        lax.broadcasted_iota(jnp.int32, (window, n_terms), 0) == place
    ).astype(f32).astype(jnp.bfloat16)

    def live(t):
        return jnp.where(t < counts_smem[0, 0], 1.0, 0.0).astype(f32)

    eye = (
        lax.broadcasted_iota(jnp.int32, (rows, LANES), 0)
        == lax.broadcasted_iota(jnp.int32, (rows, LANES), 1)
    ).astype(f32)

    def half(h):
        return slice(h * LANES, (h + 1) * LANES)

    bands = rows // SUBLANES

    def band(r):
        return pl.ds(r * SUBLANES, SUBLANES)

    def term_row(k, h, t):
        return pl.ds((k * halves + h) * tiles + t, 1)

    def spread_right(g):
        for i in range(group):
            t = g * group + i
            row = right_ref[pl.ds(t, 1), :] * live(t)
            residual_ref[pl.ds(t, 1), :] = row
            for r in range(bands):
                cols[t, band(r), :] = jnp.broadcast_to(
                    jnp.sum(eye[r * SUBLANES : (r + 1) * SUBLANES] * row, axis=1, keepdims=True),
                    (SUBLANES, LANES),
                )

    spread_right(0)

    def scatter(ref):
        full = ref[...]
        high = full.astype(jnp.bfloat16)
        low = (full - high.astype(f32)).astype(jnp.bfloat16)
        spread = jnp.dot(
            selector[...], jnp.concatenate([high, low], axis=1), preferred_element_type=f32
        )
        return (spread[:, :LANES] + spread[:, LANES:]).reshape(3 * pairs, span, LANES)

    def remote(src, dst, send, recv, device):
        return pltpu.make_async_remote_copy(
            src_ref=src, dst_ref=dst, send_sem=send, recv_sem=recv, device_id=device, device_id_type=MESH
        )

    def part_start(out_ref, in_ref, send, recv):
        def one(pos, rel, to_slab, step):
            target = lax.rem(pair + step, pairs)
            remote(
                out_ref.at[rel * pairs + target],
                in_ref.at[pos * n_sub + sub],
                send.at[pos // 2],
                recv.at[pos // 2],
                (to_slab, 2 * target + 1),
            ).start()

        for step in range(1, pairs + 1):
            pl.when(sends_far)(lambda: one(2, far_rel, far_out, step))
            one(0, 1, kept, step)
            if step < pairs:
                one(1, own_rel, slab, step)
            else:
                pl.when(rests_here)(lambda: one(1, own_rel, slab, pairs))

        @pl.when(sums_here)
        def _():
            in_ref[n_sub + sub] = out_ref[own_rel * pairs + pair]

    def field_start(src, in_ref, send, recv):
        def one(sem, rel, to_slab, step, core):
            target = 2 * lax.rem(pair + step, pairs) + core
            at = pl.multiple_of((rel * pairs + pair) * span, 8)
            remote(
                src, in_ref.at[pl.ds(at, span)], send.at[sem], recv.at[sem], (to_slab, target)
            ).start()

        for core in range(2):
            steps = range(1, pairs + 1)

            @pl.when(takes_far)
            def _():
                for step in steps:
                    one(1, kept - far_in + 1, far_in, step, core)

            for step in steps:
                one(0, 1, kept, step, core)
            for step in steps:
                if (step, core) != (pairs, 1):
                    one(0, own_rel, slab, step, core)

    def group_wait(ref, per, sem, counts, far_too, recv):
        def wait(i, count):
            size = ref.at[pl.ds(0, count * per)]
            copy = remote(size, size, sem.at[i], sem.at[i], (kept, sub))
            copy.wait_recv() if recv else copy.wait_send()

        near, far = counts
        if isinstance(near, tuple):
            pl.when(sums_here)(lambda: wait(0, near[0]))
            pl.when(rests_here)(lambda: wait(0, near[1]))
        else:
            wait(0, near)
        pl.when(far_too)(lambda: wait(1, far))

    by_pair = ((2 * pairs - 1, 2 * pairs), pairs)
    by_sub = (2 * n_sub - 1, n_sub)

    summing = slab * pairs + pair

    def from_all(it):
        return it >= ITERS - 1

    def scal_copy(it, j):
        row = scal.at[it, pl.ds(me if from_all(it) else summing, 1)]
        return remote(row, row, scal_send.at[it], scal_recv.at[it], other(j))

    def scal_start(it, row):
        scal[it, pl.ds(me if from_all(it) else summing, 1)] = row

        @pl.loop(1, n, unroll=min(n - 1, 31))
        def _(j):
            scal_copy(it, j).start()

    def scal_wait(it, count, recv):
        rest = scal.at[it, pl.ds(0, count)]
        copy = remote(rest, rest, scal_send.at[it], scal_recv.at[it], other(1))
        copy.wait_recv() if recv else copy.wait_send()

    def scal_take(it):
        if from_all(it):
            scal_wait(it, n - 1, True)
        else:
            pl.when(sums_here)(lambda: scal_wait(it, n // 2 - 1, True))
            pl.when(rests_here)(lambda: scal_wait(it, n // 2, True))

    def total(x):
        return jnp.sum(jnp.sum(x, axis=0, keepdims=True), axis=1, keepdims=True)

    lane_row = lax.broadcasted_iota(jnp.int32, (1, LANES), 1)

    def pack(parts):
        row = jnp.zeros((1, LANES), f32)
        for i, x in enumerate(parts):
            row = jnp.where(lane_row == i, total(x), row)
        return row

    def unpack(it, count):
        row = jnp.sum(scal[it][: n if from_all(it) else n // 2], axis=0, keepdims=True)
        return [
            jnp.sum(jnp.where(lane_row == i, row, 0.0), axis=1, keepdims=True)
            for i in range(count)
        ]

    def turn(x):
        rest = jnp.zeros((LANES - tiles, LANES), f32)
        return jnp.concatenate([x, rest], axis=0).T

    def gather(g):
        load(g).wait()
        pl.when(g + ahead < loads)(lambda: load(g + ahead).start())
        for i in range(group):
            t = g * group + i
            alive = live(t)
            n_sums = coupled * halves
            sums = [None] * (2 * n_sums)
            for r in range(bands):
                right = cols[t, band(r), :]
                for k in range(coupled):
                    for h in range(halves):
                        j = k * halves + h
                        a = values[t, k, band(r), half(h)]
                        sums[j] = a * right if r == 0 else sums[j] + a * right
                        sums[n_sums + j] = a * a if r == 0 else sums[n_sums + j] + a * a
            for k in range(coupled):
                for h in range(halves):
                    j = k * halves + h
                    terms[term_row(k, h, t), :] = jnp.sum(sums[j], axis=0, keepdims=True)
                    squares[term_row(k, h, t), :] = (
                        jnp.sum(sums[n_sums + j], axis=0, keepdims=True) * alive
                    )

    @pl.loop(0, loads - 1)
    def _(g):
        gather(g)
        spread_right(g + 1)

    gather(loads - 1)

    for i, ref in enumerate((terms, squares)):
        first_out[:, i] = scatter(ref)
    pl.semaphore_wait(barrier, 2 * n_sub - 1 + n_sub * fars)
    part_start(first_out, first_in, first_send, first_recv)
    pass_on(0)
    pass_on(1)
    def own_rows(ref):
        return ref[pl.ds(pl.multiple_of((n_sub + sub) * held, 8), held), :]

    def send_field(it, field):
        field_out[it] = field
        at = pl.multiple_of((own_rel * pairs + pair) * span, 8)
        field_start(field_out.at[it], field_in[it], field_send.at[it], field_recv.at[it])
        field_in[it][pl.ds(at, span), :] = field

    @pl.when(sums_here)
    def _():
        group_wait(first_in, 1, first_recv, by_sub, takes_far, True)
        sums = jnp.sum(first_in[...], axis=0)
        jacobi[...] = 1.0 / (1.0 + sums[1])
        scaled[...] = jacobi[...] * sums[0]
        kept_dir[...] = scaled[...]
        send_field(0, scaled[...])
        rho_row[...] = jnp.where(lane_row == SUMS, total(sums[0] * scaled[...]), 0.0)

    answer = jnp.zeros((held, LANES), f32)
    for it in range(ITERS):
        last = it == ITERS - 1
        fields = field_in[it]
        group_wait(fields, span, field_recv.at[it], by_pair, sends_far, True)

        def picked(t):
            alive = live(t)
            return [
                jnp.broadcast_to(
                    fields[pl.ds(wid[t, k] + h, 1), :] * alive, (SUBLANES, LANES)
                )
                for k in range(coupled)
                for h in range(halves)
            ]

        def reduced(t, r, row):
            m = None
            for k in range(coupled):
                for h in range(halves):
                    product = values[t, k, band(r), half(h)] * row[k * halves + h]
                    m = product if m is None else m + product
            return jnp.broadcast_to(jnp.sum(m, axis=1, keepdims=True), (SUBLANES, LANES))

        def forward(t):
            row = picked(t)
            for r in range(bands):
                cols[t, band(r), :] = reduced(t, r, row)

        def backward(t):
            sums = [None] * (coupled * halves)
            for r in range(bands):
                image = cols[t, band(r), :]
                for k in range(coupled):
                    for h in range(halves):
                        i = k * halves + h
                        product = values[t, k, band(r), half(h)] * image
                        sums[i] = product if r == 0 else sums[i] + product
            for k in range(coupled):
                for h in range(halves):
                    terms[term_row(k, h, t), :] = jnp.sum(
                        sums[k * halves + h], axis=0, keepdims=True
                    )

        step = divisor(tiles, STEP, 3, 2)
        if last:

            each = divisor(tiles, LAST, 3, 2)

            def turned_step(g, turned):
                for i in range(each):
                    t = g * each + i
                    row = picked(t)
                    here = lane_row == t
                    turned = [
                        jnp.where(here, reduced(t, r, row), turned[r]) for r in range(bands)
                    ]
                return turned

            image_t = turn(image)
            turned = turn(scaled_image)
            pushed = jnp.concatenate(
                lax.fori_loop(
                    0,
                    tiles // each,
                    turned_step,
                    [jnp.zeros((SUBLANES, LANES), f32)] * bands,
                ),
                axis=0,
            )
        else:
            if ORDER == 2:

                @pl.loop(0, tiles // step)
                def _(g):
                    for i in range(step):
                        forward(g * step + i)

                @pl.loop(0, tiles // step)
                def _(g):
                    for i in range(step):
                        backward(g * step + i)

            else:
                for i in range(step):
                    forward(i)

                @pl.loop(1, tiles // step)
                def _(g):
                    for i in range(step):
                        if ORDER == 0:
                            backward((g - 1) * step + i)
                        else:
                            forward(g * step + i)
                    for i in range(step):
                        if ORDER == 1:
                            backward((g - 1) * step + i)
                        else:
                            forward(g * step + i)

                for i in range(step):
                    backward(tiles - step + i)
            part_out[it] = scatter(terms)
            part_start(part_out.at[it], part_in[it], part_send.at[it], part_recv.at[it])

            @pl.loop(0, tiles, unroll=4)
            def _(t):
                rows_ref[pl.ds(t, 1), :] = jnp.sum(cols[t] * eye, axis=0, keepdims=True)

        field_own = own_rows(fields)
        if it == 0:
            for r in range(2, rounds + 1):
                pass_on(r)
            scaled_own = field_own
            direction = field_own
            scaled_image = rows_ref[...]
            image = scaled_image
        elif last:
            scal_take(ITERS)
            curve, cross = unpack(ITERS, 2)
            step_size = rho / curve
            turned = turned - step_size * pushed
            scal_start(
                it, pack((turned * turned, turned * image_t, image_t * image_t))
            )
            answer = answer + step_size * direction
            residual = residual_ref[...] - step_size * image
            scaled_own = scaled_own - step_size * field_own
            scaled_image = turned.T[:tiles]
            scal_take(it - 1)
            (square,) = unpack(it - 1, 1)
            rho_next = rho - 2.0 * step_size * cross + step_size * step_size * square
            beta = rho_next / rho
            rho = rho_next
            direction = scaled_own + beta * direction
            image = scaled_image + beta * image
        else:
            scal_take(it - 1)
            if it == 1:
                curve, cross, square, rho = unpack(it - 1, SUMS + 1)
            else:
                curve, cross, square = unpack(it - 1, SUMS)
            step_size = rho / curve
            rho_next = rho - 2.0 * step_size * cross + step_size * step_size * square
            beta = rho_next / rho
            rho = rho_next
            answer = answer + step_size * direction
            residual_ref[...] = residual_ref[...] - step_size * image
            scaled_own = scaled_own - step_size * field_own
            direction = scaled_own + beta * direction
            scaled_image = scaled_image - step_size * rows_ref[...]
            image = scaled_image + beta * image

        if it == ITERS - 2:
            scal_start(ITERS, pack((image * image, scaled_image * image)))
        if not last:

            @pl.when(sums_here)
            def _():
                if it > 0:
                    scaled[...] = scaled[...] - step_size * field_out[it]
                    kept_dir[...] = scaled[...] + beta * kept_dir[...]
                group_wait(part_in[it], 1, part_recv.at[it], by_sub, takes_far, True)
                spread = jnp.sum(part_in[it][...], axis=0)
                if it == 0:
                    scaled_back[...] = spread
                    back[...] = spread
                else:
                    scaled_back[...] = scaled_back[...] - step_size * spread
                    back[...] = scaled_back[...] + beta * back[...]
                field = jacobi[...] * back[...]
                send_field(it + 1, field)
                square = back[...] * field
                if it == ITERS - 2:
                    row = pack((square,))
                else:
                    row = pack((kept_dir[...] * back[...], scaled[...] * back[...], square))
                scal_start(it, row + rho_row[...] if it == 0 else row)

    group_wait(first_in, 1, first_send, by_pair, sends_far, False)
    for it in range(ITERS - 1):
        group_wait(part_in[it], 1, part_send.at[it], by_pair, sends_far, False)
    scal_wait(ITERS, n - 1, False)

    @pl.when(sums_here)
    def _():
        for it in range(ITERS):
            group_wait(part_in[0], 1, field_send.at[it], by_sub, takes_far, False)
        for it in range(ITERS - 1):
            scal_wait(it, n - 1, False)

    scal_take(ITERS - 1)
    new, mixed, old = unpack(ITERS - 1, SUMS)
    step_size = rho / (new + 2.0 * beta * mixed + beta * beta * old)
    answer = answer + step_size * direction
    residual_ref[...] = residual - step_size * image
    rows_ref[:held] = answer
    for h in range(halves):
        solution_ref[:, half(h)] = rows_ref[pl.ds(h, NB_DEV, stride=halves), :]

    scal_wait(ITERS - 1, n - 1, False)


def per_device(n_slab, n_sub, values, block_ids, tile_counts, right_side):
    tiles, coupled, rows, block = values.shape
    halves = block // LANES
    held = NB_DEV * halves
    n = n_slab * n_sub
    slots = 3 * n_sub
    window = slots * held
    span = 2 * held
    pairs = n_sub // 2
    n_terms = round_up(tiles * coupled * halves, LANES)
    loads = tiles // divisor(tiles, GROUP, 3, 2)
    f32 = jnp.float32
    vmem = pltpu.VMEM
    dma = pltpu.SemaphoreType.DMA
    whole = pl.BlockSpec(memory_space=pltpu.VMEM)
    return pl.pallas_call(
        functools.partial(kernel, n_slab, n_sub),
        out_shape=(
            jax.ShapeDtypeStruct((NB_DEV, block), f32),
            jax.ShapeDtypeStruct((tiles, rows), f32),
        ),
        in_specs=[pl.BlockSpec(memory_space=pltpu.HBM)] * 4,
        out_specs=(whole, whole),
        scratch_shapes=[
            vmem(values.shape, f32),
            pltpu.SMEM((tiles, coupled), jnp.int32),
            vmem((window, n_terms), jnp.bfloat16),
            vmem((n_terms, LANES), f32),
            vmem((n_terms, LANES), f32),
            vmem((tiles, rows, LANES), f32),
            vmem((tiles, LANES), f32),
            vmem((3 * pairs, 2, span, LANES), f32),
            vmem((slots, 2, span, LANES), f32),
            vmem((ITERS - 1, 3 * pairs, span, LANES), f32),
            [vmem((slots, span, LANES), f32)] * (ITERS - 1),
            vmem((ITERS, span, LANES), f32),
            [vmem((window, LANES), f32)] * ITERS,
            vmem((ITERS + 1, n, LANES), f32),
            pltpu.SMEM((coupled, tiles), jnp.int32),
            pltpu.SMEM((1, 1), jnp.int32),
            vmem((tiles, rows), f32),
            dma((3,)),
            dma((loads,)),
            dma((2,)),
            dma((2,)),
            dma((ITERS - 1, 2)),
            dma((ITERS - 1, 2)),
            dma((ITERS, 2)),
            dma((ITERS, 2)),
            dma((ITERS + 1,)),
            dma((ITERS + 1,)),
            pltpu.SemaphoreType.REGULAR((max(1, n_slab // 2 - 1),)),
            *([vmem((span, LANES), f32)] * 5),
            vmem((1, LANES), f32),
        ],
        compiler_params=pltpu.CompilerParams(
            collective_id=0, has_side_effects=True, vmem_limit_bytes=48 * 1024 * 1024
        ),
    )(values, pltpu.with_memory_space_constraint(block_ids.T, pltpu.HBM), tile_counts, pltpu.with_memory_space_constraint(right_side, pltpu.HBM))


def solution(mesh):
    in_specs = (
        P(("slab", "sub"), None, None, None),
        P(("slab", "sub"), None),
        P("slab", "sub"),
        P(("slab", "sub"), None),
    )
    out_specs = (P(("slab", "sub"), None), P(("slab", "sub"), None))
    return jax.shard_map(
        functools.partial(per_device, mesh.shape["slab"], mesh.shape["sub"]),
        mesh=mesh,
        in_specs=in_specs,
        out_specs=out_specs,
        check_vma=False,
    )
```

```python
import functools

import jax
import jax.numpy as jnp
from jax import lax
from jax.experimental import pallas as pl
from jax.experimental.pallas import tpu as pltpu
from jax.sharding import PartitionSpec as P

ITERS = 4
NB_DEV = 12
LANES = 128
SUMS = 3
STEP = 12
ORDER = 2
LAST = 24
AHEAD = 4
GROUP = 4
SUBLANES = 8
MESH = pl.DeviceIdType.MESH


def round_up(size, unit):
    return -(-size // unit) * unit


def divisor(size, *wanted):
    return next(g for g in (*wanted, 1) if size % g == 0)


def kernel(
    n_slab,
    n_sub,
    values_hbm,
    ids_hbm,
    counts_hbm,
    right_hbm,
    solution_ref,
    residual_ref,
    values,
    wid,
    selector,
    terms,
    squares,
    cols,
    rows_ref,
    first_out,
    first_in,
    part_out,
    part_in,
    field_out,
    field_in,
    scal,
    ids_smem,
    counts_smem,
    right_ref,
    small_sem,
    load_sem,
    first_send,
    first_recv,
    part_send,
    part_recv,
    field_send,
    field_recv,
    scal_send,
    scal_recv,
    hello,
    jacobi,
    scaled,
    kept_dir,
    scaled_back,
    back,
    rho_row,
):
    tiles, coupled, rows, block = values.shape
    halves = block // LANES
    held = NB_DEV * halves
    n = n_slab * n_sub
    window = 3 * n_sub * held
    n_terms = terms.shape[0]
    f32 = jnp.float32
    slab = lax.axis_index("slab")
    sub = lax.axis_index("sub")
    me = slab * n_sub + sub
    pairs = n_sub // 2
    span = 2 * held
    pair = lax.div(sub, 2)
    sums_here = lax.rem(sub, 2) == 1
    rests_here = lax.rem(sub, 2) == 0

    kept = slab + 1 - 2 * lax.rem(slab, 2)
    own_rel = kept - slab + 1
    beyond = 2 * slab - kept
    far_rel = slab - kept + 1
    far_out = 3 * slab - 2 * kept
    far_in = 2 * kept - slab
    sends_far = jnp.logical_and(beyond >= 0, beyond < n_slab)
    takes_far = jnp.logical_and(far_in >= 0, far_in < n_slab)

    small = [
        pltpu.make_async_copy(src, dst, small_sem.at[i])
        for i, (src, dst) in enumerate(
            ((ids_hbm, ids_smem), (counts_hbm, counts_smem), (right_hbm, right_ref))
        )
    ]
    for copy in small:
        copy.start()
    loads = load_sem.shape[0]
    group = tiles // loads

    def load(g):
        part = pl.ds(g * group, group)
        return pltpu.make_async_copy(values_hbm.at[part], values.at[part], load_sem.at[g])

    ahead = min(AHEAD, loads)
    for g in range(ahead):
        load(g).start()

    def other(j):
        target = lax.rem(me + j, n)
        return (lax.div(target, n_sub), lax.rem(target, n_sub))

    barrier = pltpu.get_barrier_semaphore()

    def greet(slot, to_slab, target):
        pl.semaphore_signal(slot, inc=1, device_id=(to_slab, target), device_id_type=MESH)

    for exists, to_slab in ((sends_far, far_out), (takes_far, far_in)):

        @pl.when(exists)
        def _():
            for step in range(n_sub):
                greet(barrier, to_slab, lax.rem(sub + step, n_sub))

    for step in range(n_sub):
        greet(barrier, kept, lax.rem(sub + step, n_sub))
    for step in range(1, n_sub):
        greet(barrier, slab, lax.rem(sub + step, n_sub))

    fars = sends_far.astype(jnp.int32) + takes_far.astype(jnp.int32)
    rounds = hello.shape[0]

    def pass_on(r):
        if r > 0:
            pl.semaphore_wait(hello.at[r - 1], fars)
        if r < rounds:
            pl.when(sends_far)(lambda: greet(hello.at[r], far_out, sub))
            pl.when(takes_far)(lambda: greet(hello.at[r], far_in, sub))

    n_used = tiles * coupled * halves
    if n_terms > n_used:
        terms[n_used:] = jnp.zeros((n_terms - n_used, LANES), f32)
        squares[n_used:] = jnp.zeros((n_terms - n_used, LANES), f32)

    @pl.when(jnp.logical_not(takes_far))
    def _():
        for ref in (*first_in, *part_in):
            ref[2 * n_sub :] = jnp.zeros((n_sub,) + ref.shape[1:], f32)

    @pl.when(jnp.logical_not(sends_far))
    def _():
        blank = pl.ds(pl.multiple_of(far_rel * n_sub * held, 8), n_sub * held)
        for ref in field_in:
            ref[blank, :] = jnp.zeros((n_sub * held, LANES), f32)

    for copy in small:
        copy.wait()

    base = (slab - 1) * n_sub * NB_DEV
    lane = lax.broadcasted_iota(jnp.int32, (1, n_terms), 1)
    lane_tile = lane % tiles
    lane_k = lane // (halves * tiles)
    lane_h = (lane // tiles) % halves
    place = jnp.full((1, n_terms), -1, jnp.int32)
    for t in range(tiles):
        for k in range(coupled):
            at = jnp.clip((ids_smem[k, t] - base) * halves, 0, window - halves)
            wid[t, k] = at
            place = jnp.where(jnp.logical_and(lane_tile == t, lane_k == k), at + lane_h, place)
    selector[...] = (
        lax.broadcasted_iota(jnp.int32, (window, n_terms), 0) == place
    ).astype(f32).astype(jnp.bfloat16)

    def live(t):
        return jnp.where(t < counts_smem[0, 0], 1.0, 0.0).astype(f32)

    eye = (
        lax.broadcasted_iota(jnp.int32, (rows, LANES), 0)
        == lax.broadcasted_iota(jnp.int32, (rows, LANES), 1)
    ).astype(f32)

    def half(h):
        return slice(h * LANES, (h + 1) * LANES)

    bands = rows // SUBLANES

    def band(r):
        return pl.ds(r * SUBLANES, SUBLANES)

    def term_row(k, h, t):
        return pl.ds((k * halves + h) * tiles + t, 1)

    def spread_right(g):
        for i in range(group):
            t = g * group + i
            row = right_ref[pl.ds(t, 1), :] * live(t)
            residual_ref[pl.ds(t, 1), :] = row
            for r in range(bands):
                cols[t, band(r), :] = jnp.broadcast_to(
                    jnp.sum(eye[r * SUBLANES : (r + 1) * SUBLANES] * row, axis=1, keepdims=True),
                    (SUBLANES, LANES),
                )

    spread_right(0)

    def scatter(ref):
        full = ref[...]
        high = full.astype(jnp.bfloat16)
        low = (full - high.astype(f32)).astype(jnp.bfloat16)
        spread = jnp.dot(
            selector[...], jnp.concatenate([high, low], axis=1), preferred_element_type=f32
        )
        return (spread[:, :LANES] + spread[:, LANES:]).reshape(3 * pairs, span, LANES)

    def remote(src, dst, send, recv, device):
        return pltpu.make_async_remote_copy(
            src_ref=src, dst_ref=dst, send_sem=send, recv_sem=recv, device_id=device, device_id_type=MESH
        )

    def part_start(out_ref, in_ref, send, recv):
        def one(pos, rel, to_slab, step):
            target = lax.rem(pair + step, pairs)
            remote(
                out_ref.at[rel * pairs + target],
                in_ref.at[pos * n_sub + sub],
                send.at[pos // 2],
                recv.at[pos // 2],
                (to_slab, 2 * target + 1),
            ).start()

        for step in range(1, pairs + 1):
            pl.when(sends_far)(lambda: one(2, far_rel, far_out, step))
            one(0, 1, kept, step)
            if step < pairs:
                one(1, own_rel, slab, step)
            else:
                pl.when(rests_here)(lambda: one(1, own_rel, slab, pairs))

        @pl.when(sums_here)
        def _():
            in_ref[n_sub + sub] = out_ref[own_rel * pairs + pair]

    def field_start(src, in_ref, send, recv):
        def one(sem, rel, to_slab, step, core):
            target = 2 * lax.rem(pair + step, pairs) + core
            at = pl.multiple_of((rel * pairs + pair) * span, 8)
            remote(
                src, in_ref.at[pl.ds(at, span)], send.at[sem], recv.at[sem], (to_slab, target)
            ).start()

        for core in range(2):
            steps = range(1, pairs + 1)

            @pl.when(takes_far)
            def _():
                for step in steps:
                    one(1, kept - far_in + 1, far_in, step, core)

            for step in steps:
                one(0, 1, kept, step, core)
            for step in steps:
                if (step, core) != (pairs, 1):
                    one(0, own_rel, slab, step, core)

    def group_wait(ref, per, sem, counts, far_too, recv):
        def wait(i, count):
            size = ref.at[pl.ds(0, count * per)]
            copy = remote(size, size, sem.at[i], sem.at[i], (kept, sub))
            copy.wait_recv() if recv else copy.wait_send()

        near, far = counts
        if isinstance(near, tuple):
            pl.when(sums_here)(lambda: wait(0, near[0]))
            pl.when(rests_here)(lambda: wait(0, near[1]))
        else:
            wait(0, near)
        pl.when(far_too)(lambda: wait(1, far))

    by_pair = ((2 * pairs - 1, 2 * pairs), pairs)
    by_sub = (2 * n_sub - 1, n_sub)

    summing = slab * pairs + pair

    def from_all(it):
        return it >= ITERS - 1

    def scal_copy(it, j):
        row = scal.at[it, pl.ds(me if from_all(it) else summing, 1)]
        return remote(row, row, scal_send.at[it], scal_recv.at[it], other(j))

    def scal_start(it, row):
        scal[it, pl.ds(me if from_all(it) else summing, 1)] = row

        @pl.loop(1, n, unroll=min(n - 1, 31))
        def _(j):
            scal_copy(it, j).start()

    def scal_wait(it, count, recv):
        rest = scal.at[it, pl.ds(0, count)]
        copy = remote(rest, rest, scal_send.at[it], scal_recv.at[it], other(1))
        copy.wait_recv() if recv else copy.wait_send()

    def scal_take(it):
        if from_all(it):
            scal_wait(it, n - 1, True)
        else:
            pl.when(sums_here)(lambda: scal_wait(it, n // 2 - 1, True))
            pl.when(rests_here)(lambda: scal_wait(it, n // 2, True))

    def total(x):
        return jnp.sum(jnp.sum(x, axis=0, keepdims=True), axis=1, keepdims=True)

    lane_row = lax.broadcasted_iota(jnp.int32, (1, LANES), 1)

    def pack(parts):
        row = jnp.zeros((1, LANES), f32)
        for i, x in enumerate(parts):
            row = jnp.where(lane_row == i, total(x), row)
        return row

    def unpack(it, count):
        row = jnp.sum(scal[it][: n if from_all(it) else n // 2], axis=0, keepdims=True)
        return [
            jnp.sum(jnp.where(lane_row == i, row, 0.0), axis=1, keepdims=True)
            for i in range(count)
        ]

    def turn(x):
        rest = jnp.zeros((LANES - tiles, LANES), f32)
        return jnp.concatenate([x, rest], axis=0).T

    def gather(g):
        load(g).wait()
        pl.when(g + ahead < loads)(lambda: load(g + ahead).start())
        for i in range(group):
            t = g * group + i
            alive = live(t)
            n_sums = coupled * halves
            sums = [None] * (2 * n_sums)
            for r in range(bands):
                right = cols[t, band(r), :]
                for k in range(coupled):
                    for h in range(halves):
                        j = k * halves + h
                        a = values[t, k, band(r), half(h)]
                        sums[j] = a * right if r == 0 else sums[j] + a * right
                        sums[n_sums + j] = a * a if r == 0 else sums[n_sums + j] + a * a
            for k in range(coupled):
                for h in range(halves):
                    j = k * halves + h
                    terms[term_row(k, h, t), :] = jnp.sum(sums[j], axis=0, keepdims=True)
                    squares[term_row(k, h, t), :] = (
                        jnp.sum(sums[n_sums + j], axis=0, keepdims=True) * alive
                    )

    @pl.loop(0, loads - 1)
    def _(g):
        gather(g)
        spread_right(g + 1)

    gather(loads - 1)

    pl.semaphore_wait(barrier, 2 * n_sub - 1 + n_sub * fars)
    for i, ref in enumerate((terms, squares)):
        first_out[i][...] = scatter(ref)
        part_start(first_out[i], first_in[i], first_send.at[i], first_recv.at[i])
    pass_on(0)
    pass_on(1)
    def own_rows(ref):
        return ref[pl.ds(pl.multiple_of((n_sub + sub) * held, 8), held), :]

    def send_field(it, field):
        field_out[it] = field
        at = pl.multiple_of((own_rel * pairs + pair) * span, 8)
        field_start(field_out.at[it], field_in[it], field_send.at[it], field_recv.at[it])
        field_in[it][pl.ds(at, span), :] = field

    @pl.when(sums_here)
    def _():
        for i in range(2):
            group_wait(first_in[i], 1, first_recv.at[i], by_sub, takes_far, True)
        sums = [jnp.sum(ref[...], axis=0) for ref in first_in]
        jacobi[...] = 1.0 / (1.0 + sums[1])
        scaled[...] = jacobi[...] * sums[0]
        kept_dir[...] = scaled[...]
        send_field(0, scaled[...])
        rho_row[...] = jnp.where(lane_row == SUMS, total(sums[0] * scaled[...]), 0.0)

    answer = jnp.zeros((held, LANES), f32)
    for it in range(ITERS):
        last = it == ITERS - 1
        fields = field_in[it]
        group_wait(fields, span, field_recv.at[it], by_pair, sends_far, True)

        def picked(t):
            alive = live(t)
            return [
                jnp.broadcast_to(
                    fields[pl.ds(wid[t, k] + h, 1), :] * alive, (SUBLANES, LANES)
                )
                for k in range(coupled)
                for h in range(halves)
            ]

        def reduced(t, r, row):
            m = None
            for k in range(coupled):
                for h in range(halves):
                    product = values[t, k, band(r), half(h)] * row[k * halves + h]
                    m = product if m is None else m + product
            return jnp.broadcast_to(jnp.sum(m, axis=1, keepdims=True), (SUBLANES, LANES))

        def forward(t):
            row = picked(t)
            for r in range(bands):
                cols[t, band(r), :] = reduced(t, r, row)

        def backward(t):
            sums = [None] * (coupled * halves)
            for r in range(bands):
                image = cols[t, band(r), :]
                for k in range(coupled):
                    for h in range(halves):
                        i = k * halves + h
                        product = values[t, k, band(r), half(h)] * image
                        sums[i] = product if r == 0 else sums[i] + product
            for k in range(coupled):
                for h in range(halves):
                    terms[term_row(k, h, t), :] = jnp.sum(
                        sums[k * halves + h], axis=0, keepdims=True
                    )

        step = divisor(tiles, STEP, 3, 2)
        if last:

            each = divisor(tiles, LAST, 3, 2)

            def turned_step(g, turned):
                for i in range(each):
                    t = g * each + i
                    row = picked(t)
                    here = lane_row == t
                    turned = [
                        jnp.where(here, reduced(t, r, row), turned[r]) for r in range(bands)
                    ]
                return turned

            image_t = turn(image)
            turned = turn(scaled_image)
            pushed = jnp.concatenate(
                lax.fori_loop(
                    0,
                    tiles // each,
                    turned_step,
                    [jnp.zeros((SUBLANES, LANES), f32)] * bands,
                ),
                axis=0,
            )
        else:
            if ORDER == 2:

                @pl.loop(0, tiles // step)
                def _(g):
                    for i in range(step):
                        forward(g * step + i)

                @pl.loop(0, tiles // step)
                def _(g):
                    for i in range(step):
                        backward(g * step + i)

            else:
                for i in range(step):
                    forward(i)

                @pl.loop(1, tiles // step)
                def _(g):
                    for i in range(step):
                        if ORDER == 0:
                            backward((g - 1) * step + i)
                        else:
                            forward(g * step + i)
                    for i in range(step):
                        if ORDER == 1:
                            backward((g - 1) * step + i)
                        else:
                            forward(g * step + i)

                for i in range(step):
                    backward(tiles - step + i)
            part_out[it] = scatter(terms)
            part_start(part_out.at[it], part_in[it], part_send.at[it], part_recv.at[it])

            @pl.loop(0, tiles, unroll=4)
            def _(t):
                rows_ref[pl.ds(t, 1), :] = jnp.sum(cols[t] * eye, axis=0, keepdims=True)

        field_own = own_rows(fields)
        if it == 0:
            for r in range(2, rounds + 1):
                pass_on(r)
            scaled_own = field_own
            direction = field_own
            scaled_image = rows_ref[...]
            image = scaled_image
        elif last:
            scal_take(ITERS)
            curve, cross = unpack(ITERS, 2)
            step_size = rho / curve
            turned = turned - step_size * pushed
            scal_start(
                it, pack((turned * turned, turned * image_t, image_t * image_t))
            )
            answer = answer + step_size * direction
            residual = residual_ref[...] - step_size * image
            scaled_own = scaled_own - step_size * field_own
            scaled_image = turned.T[:tiles]
            scal_take(it - 1)
            (square,) = unpack(it - 1, 1)
            rho_next = rho - 2.0 * step_size * cross + step_size * step_size * square
            beta = rho_next / rho
            rho = rho_next
            direction = scaled_own + beta * direction
            image = scaled_image + beta * image
        else:
            scal_take(it - 1)
            if it == 1:
                curve, cross, square, rho = unpack(it - 1, SUMS + 1)
            else:
                curve, cross, square = unpack(it - 1, SUMS)
            step_size = rho / curve
            rho_next = rho - 2.0 * step_size * cross + step_size * step_size * square
            beta = rho_next / rho
            rho = rho_next
            answer = answer + step_size * direction
            residual_ref[...] = residual_ref[...] - step_size * image
            scaled_own = scaled_own - step_size * field_own
            direction = scaled_own + beta * direction
            scaled_image = scaled_image - step_size * rows_ref[...]
            image = scaled_image + beta * image

        if it == ITERS - 2:
            scal_start(ITERS, pack((image * image, scaled_image * image)))
        if not last:

            @pl.when(sums_here)
            def _():
                if it > 0:
                    scaled[...] = scaled[...] - step_size * field_out[it]
                    kept_dir[...] = scaled[...] + beta * kept_dir[...]
                group_wait(part_in[it], 1, part_recv.at[it], by_sub, takes_far, True)
                spread = jnp.sum(part_in[it][...], axis=0)
                if it == 0:
                    scaled_back[...] = spread
                    back[...] = spread
                else:
                    scaled_back[...] = scaled_back[...] - step_size * spread
                    back[...] = scaled_back[...] + beta * back[...]
                field = jacobi[...] * back[...]
                send_field(it + 1, field)
                square = back[...] * field
                if it == ITERS - 2:
                    row = pack((square,))
                else:
                    row = pack((kept_dir[...] * back[...], scaled[...] * back[...], square))
                scal_start(it, row + rho_row[...] if it == 0 else row)

    for i in range(2):
        group_wait(first_in[i], 1, first_send.at[i], by_pair, sends_far, False)
    for it in range(ITERS - 1):
        group_wait(part_in[it], 1, part_send.at[it], by_pair, sends_far, False)
    scal_wait(ITERS, n - 1, False)

    @pl.when(sums_here)
    def _():
        for it in range(ITERS):
            group_wait(part_in[0], 1, field_send.at[it], by_sub, takes_far, False)
        for it in range(ITERS - 1):
            scal_wait(it, n - 1, False)

    scal_take(ITERS - 1)
    new, mixed, old = unpack(ITERS - 1, SUMS)
    step_size = rho / (new + 2.0 * beta * mixed + beta * beta * old)
    answer = answer + step_size * direction
    residual_ref[...] = residual - step_size * image
    rows_ref[:held] = answer
    for h in range(halves):
        solution_ref[:, half(h)] = rows_ref[pl.ds(h, NB_DEV, stride=halves), :]

    scal_wait(ITERS - 1, n - 1, False)


def per_device(n_slab, n_sub, values, block_ids, tile_counts, right_side):
    tiles, coupled, rows, block = values.shape
    halves = block // LANES
    held = NB_DEV * halves
    n = n_slab * n_sub
    slots = 3 * n_sub
    window = slots * held
    span = 2 * held
    pairs = n_sub // 2
    n_terms = round_up(tiles * coupled * halves, LANES)
    loads = tiles // divisor(tiles, GROUP, 3, 2)
    f32 = jnp.float32
    vmem = pltpu.VMEM
    dma = pltpu.SemaphoreType.DMA
    whole = pl.BlockSpec(memory_space=pltpu.VMEM)
    return pl.pallas_call(
        functools.partial(kernel, n_slab, n_sub),
        out_shape=(
            jax.ShapeDtypeStruct((NB_DEV, block), f32),
            jax.ShapeDtypeStruct((tiles, rows), f32),
        ),
        in_specs=[pl.BlockSpec(memory_space=pltpu.HBM)] * 4,
        out_specs=(whole, whole),
        scratch_shapes=[
            vmem(values.shape, f32),
            pltpu.SMEM((tiles, coupled), jnp.int32),
            vmem((window, n_terms), jnp.bfloat16),
            vmem((n_terms, LANES), f32),
            vmem((n_terms, LANES), f32),
            vmem((tiles, rows, LANES), f32),
            vmem((tiles, LANES), f32),
            [vmem((3 * pairs, span, LANES), f32)] * 2,
            [vmem((slots, span, LANES), f32)] * 2,
            vmem((ITERS - 1, 3 * pairs, span, LANES), f32),
            [vmem((slots, span, LANES), f32)] * (ITERS - 1),
            vmem((ITERS, span, LANES), f32),
            [vmem((window, LANES), f32)] * ITERS,
            vmem((ITERS + 1, n, LANES), f32),
            pltpu.SMEM((coupled, tiles), jnp.int32),
            pltpu.SMEM((1, 1), jnp.int32),
            vmem((tiles, rows), f32),
            dma((3,)),
            dma((loads,)),
            dma((2, 2)),
            dma((2, 2)),
            dma((ITERS - 1, 2)),
            dma((ITERS - 1, 2)),
            dma((ITERS, 2)),
            dma((ITERS, 2)),
            dma((ITERS + 1,)),
            dma((ITERS + 1,)),
            pltpu.SemaphoreType.REGULAR((max(1, n_slab // 2 - 1),)),
            *([vmem((span, LANES), f32)] * 5),
            vmem((1, LANES), f32),
        ],
        compiler_params=pltpu.CompilerParams(
            collective_id=0, has_side_effects=True, vmem_limit_bytes=48 * 1024 * 1024
        ),
    )(values, pltpu.with_memory_space_constraint(block_ids.T, pltpu.HBM), tile_counts, pltpu.with_memory_space_constraint(right_side, pltpu.HBM))


def solution(mesh):
    in_specs = (
        P(("slab", "sub"), None, None, None),
        P(("slab", "sub"), None),
        P("slab", "sub"),
        P(("slab", "sub"), None),
    )
    out_specs = (P(("slab", "sub"), None), P(("slab", "sub"), None))
    return jax.shard_map(
        functools.partial(per_device, mesh.shape["slab"], mesh.shape["sub"]),
        mesh=mesh,
        in_specs=in_specs,
        out_specs=out_specs,
        check_vma=False,
    )
```
